32 devices in a mesh: ta: 8 (over y, x, core), sa: 4 (over z).
Axes of the slice: x: 2, y: 2, z: 4, core: 2. Of those that a mesh axis runs over, the one named last changes fastest.
Arguments:
- eigenvectors: bfloat16 [8, 256, 2, 3, 4, 384], P('ta', None, None, None, 'sa'), may hold values from -17 to 17
- momenta: int32 [8, 3], replicated, may hold values from -4 to 4
- block_order: int32 [4], replicated, may hold values from 0 to 3, each once
Outputs:
- meson_fields: float32 [8, 16, 64, 8, 128], P(None, 'sa', 'ta')
- slice_norms: float32 [8, 256], P('ta')
The draws below stay inside these ranges and needn't reach their ends.
Inputs may be any that keep to these rules, and one draw needn't show every extreme that they name: block_order names every block once.
All inputs are finite; a program needn't handle non-finite values.
Results may differ from the reference program's by a relative error of at most 0.0018.
Values sent between devices are 32-bit elements; how exact they have to be, the bound alone decides.
A program may use at most 64 MiB of HBM per device.

```python
import math
import jax
import jax.numpy as jnp
from jax import lax

NC = 3
BS = 64
NBLK = 4
P_SIZE = 8
LX = 96
NV = 256
NT = 8
NZ = 4
PLANE = 384


def draw_eigenvectors(key, part):
    gauss_key, rough_key = jax.random.split(jax.random.fold_in(key, 17), 2)
    full_shape = (NT, NV, 2, NC, NZ, PLANE)
    roughness = jax.random.uniform(rough_key, (NT, 1, 1, 1, NZ, PLANE), jnp.float32, 0.7, 1.4)
    height = jnp.arange(NZ, dtype=jnp.float32) / max(NZ - 1, 1)
    rising = jnp.sqrt(1.0 + 2.0 * height).reshape(1, 1, 1, 1, NZ, 1)
    values = jnp.clip(jax.random.normal(gauss_key, full_shape, jnp.float32), -4.0, 4.0)
    return (values * roughness * rising).astype(jnp.bfloat16)


def place_ends(array, key, least, top_value):
    shape = array.shape
    index_at = [jax.random.randint(jax.random.fold_in(key, axis), (), 0, shape[axis]) for axis in range(len(shape))]
    array = array.at[tuple(index_at)].set(least)
    longest = shape.index(max(shape))
    index_at[longest] = (index_at[longest] + 1) % shape[longest]
    return array.at[tuple(index_at)].set(top_value)


def setup_inputs(seed: int = 0) -> dict:
    key_of = jax.random.split(jax.random.key(seed), 4)
    return {
        "eigenvectors": draw_eigenvectors(jax.random.fold_in(key_of[3], 71), 0),
        "momenta": place_ends(jax.random.randint(key_of[1], (P_SIZE, 3), -4, 5), jax.random.fold_in(key_of[1], 1), -4, 4).astype(jnp.int32),
        "block_order": jax.random.permutation(key_of[2], NBLK).astype(jnp.int32),
    }


full_turn = 2.0 * math.pi

def phased_right(blocks, cos_table, sin_table):
    real_part = blocks[:, :, 0].astype(jnp.float32)[None]
    imag_part = blocks[:, :, 1].astype(jnp.float32)[None]
    cos_full = cos_table[:, None, None, None, :]
    sin_full = sin_table[:, None, None, None, :]
    phased_re = (real_part * cos_full + imag_part * sin_full).astype(jnp.bfloat16)
    phased_im = (imag_part * cos_full - real_part * sin_full).astype(jnp.bfloat16)
    first_half = jnp.stack([phased_re, phased_im], axis=3)
    second_half = jnp.stack([phased_im, -phased_re], axis=3)
    right_cols = jnp.stack([first_half, second_half], axis=1)
    return right_cols.reshape(right_cols.shape[0], 2, right_cols.shape[2], right_cols.shape[3], -1)

def reference(eigenvectors, momenta, block_order):
    site_count = NZ * PLANE
    site_index = jnp.arange(site_count, dtype=jnp.int32)
    z_coord = site_index // PLANE
    within_plane = site_index % PLANE
    x_coord = within_plane % LX
    y_coord = within_plane // LX
    phase_index = momenta[:, 0:1] * x_coord[None, :] + momenta[:, 1:2] * y_coord[None, :] + momenta[:, 2:3] * z_coord[None, :]
    phase_index = jnp.mod(phase_index, LX).astype(jnp.int32)
    angles = phase_index.astype(jnp.float32) * (full_turn / LX)
    cosines = jnp.cos(angles)[:, None, :]
    sine_vals = jnp.sin(angles)[:, None, :]
    norm_scale = 1.0 / math.sqrt(2 * NC * NZ * PLANE)

    def one_slice(slab_data):
        blocks = slab_data.reshape(NBLK, BS, 2, NC, site_count)
        ordered = jnp.take(blocks, block_order, axis=0)
        left_rows = ordered.reshape(NBLK, BS, 2 * NC * site_count).astype(jnp.float32)

        def one_momentum(trig_pair):
            right_cols = phased_right(ordered, trig_pair[0], trig_pair[1])[0]
            product = jnp.einsum('ark,cbjk->abrcj', left_rows, right_cols.astype(jnp.float32))
            return product.reshape(NBLK * NBLK, BS, 2 * BS)
        fields = lax.map(one_momentum, (cosines, sine_vals))
        squares = lax.optimization_barrier(jnp.sum(jnp.square(slab_data.astype(jnp.float32)), axis=(1, 2, 3, 4)))
        return (fields, squares)
    fields, squares = lax.map(one_slice, eigenvectors)
    meson_fields = jnp.transpose(fields, (1, 2, 3, 0, 4)) * norm_scale
    slice_norms = squares / (2 * NC * NZ * PLANE)
    return (meson_fields, slice_norms)
```

```python
import functools
import math

import jax
import jax.numpy as jnp
from jax import lax
from jax.experimental import pallas as pl
from jax.experimental.pallas import tpu as pltpu
from jax.sharding import PartitionSpec as P

NC = 3
BS = 64
NBLK = 4
LX = 96
MESH = pl.DeviceIdType.MESH

full_turn = 2.0 * math.pi


def line_kernel(
    n, nta, scale, inv_count,
    order_ref, momenta_ref, ev_ref,
    out_ref, norm_ref,
    left, right, parts, rbuf, lbuf, final, recv, nbuf,
    rsend, rrecv, lsend, lrecv, asend, arecv, nsend, nrecv,
):
    t, z = lax.axis_index("ta"), lax.axis_index("sa")
    moms, planes = momenta_ref.shape[1], ev_ref.shape[-1]
    ppd = NBLK * NBLK // n
    rows = BS // nta
    half = NC * planes

    barrier = pltpu.get_barrier_semaphore()
    for j in range(1, n):
        pl.semaphore_signal(barrier, inc=1, device_id={"sa": lax.rem(z + j, n)}, device_id_type=MESH)
    for j in range(1, nta):
        pl.semaphore_signal(barrier, inc=1, device_id={"ta": lax.rem(t + j, nta)}, device_id_type=MESH)

    for b in range(NBLK):
        stored = order_ref[b]
        for k in range(2 * NC):
            left[b * BS:(b + 1) * BS, k * planes:(k + 1) * planes] = ev_ref[k, stored]
    def norm_copy(peer, slot):
        return pltpu.make_async_remote_copy(
            src_ref=nbuf.at[slot], dst_ref=nbuf.at[slot], send_sem=nsend.at[peer], recv_sem=nrecv.at[slot],
            device_id={"sa": peer}, device_id_type=MESH,
        )

    def shard(ref, p, s):
        return ref.at[p, pl.ds(s * ppd, ppd)]

    def rightward(src, p, s):
        return pltpu.make_async_remote_copy(
            src_ref=shard(src, p, s), dst_ref=shard(rbuf, p, s), send_sem=rsend.at[p, s], recv_sem=rrecv.at[p, s],
            device_id={"sa": lax.rem(z + 1, n)}, device_id_type=MESH,
        )

    def leftward(src, p, s):
        return pltpu.make_async_remote_copy(
            src_ref=shard(src, p, s), dst_ref=shard(lbuf, p, s), send_sem=lsend.at[p, s], recv_sem=lrecv.at[p, s],
            device_id={"sa": lax.rem(z + n - 1, n)}, device_id_type=MESH,
        )

    def compute(p):
        site = lax.broadcasted_iota(jnp.int32, (1, planes), 1)
        phase_index = (
            momenta_ref[0, p] * lax.rem(site, LX)
            + momenta_ref[1, p] * lax.div(site, LX)
            + momenta_ref[2, p] * z
        )
        angles = jnp.mod(phase_index, LX).astype(jnp.float32) * (full_turn / LX)
        cosine, sine = jnp.cos(angles), jnp.sin(angles)
        for c in range(NC):
            lanes = slice(c * planes, (c + 1) * planes)
            upper = slice(half + c * planes, half + (c + 1) * planes)
            for b in range(NBLK):
                re = left[b * BS:(b + 1) * BS, lanes].astype(jnp.float32)
                im = left[b * BS:(b + 1) * BS, upper].astype(jnp.float32)
                phased_re = (re * cosine + im * sine).astype(jnp.bfloat16)
                phased_im = (im * cosine - re * sine).astype(jnp.bfloat16)
                first = slice(2 * b * BS, (2 * b + 1) * BS)
                second = slice((2 * b + 1) * BS, (2 * b + 2) * BS)
                right[first, lanes] = phased_re
                right[first, upper] = phased_im
                right[second, lanes] = phased_im
                right[second, upper] = -phased_re
        for pair in range(NBLK // 2):
            product = lax.dot_general(
                left[...], right[pair * 4 * BS:(pair + 1) * 4 * BS, :], (((1,), (1,)), ((), ())),
                preferred_element_type=jnp.float32,
            )
            for a in range(NBLK):
                for b in range(2):
                    parts[p, a * NBLK + 2 * pair + b] = product[a * BS:(a + 1) * BS, b * 2 * BS:(b + 1) * 2 * BS]

    def open_lines(slot):
        @pl.when(z == 0)
        def _():
            for s in range(n - 1, 0, -1):
                p = slot - (n - 1 - s)

                @pl.when((p >= 0) & (p < moms))
                def _():
                    rightward(parts, p, s).start()

        @pl.when(z == n - 1)
        def _():
            for s in range(n - 1):
                p = slot - s

                @pl.when((p >= 0) & (p < moms))
                def _():
                    leftward(parts, p, s).start()

    def compute_and_open(p, carry):
        compute(p)
        open_lines(p)
        return carry

    def only_open(slot, carry):
        open_lines(slot)
        return carry

    compute(0)
    pl.semaphore_wait(barrier, n - 1 + nta - 1)
    open_lines(0)
    lax.fori_loop(1, moms, compute_and_open, 0)
    lax.fori_loop(moms, moms + n - 2, only_open, 0)

    squares = []
    for b in range(NBLK):
        total = jnp.zeros((BS, 128), jnp.float32)
        for k in range(2 * NC):
            for lane in range(0, planes, 128):
                value = ev_ref[k, b, :, lane:lane + 128].astype(jnp.float32)
                total = total + value * value
        squares.append(total)
    nbuf[z] = lax.dot_general(
        jnp.ones((8, 128), jnp.float32), jnp.concatenate(squares, axis=0), (((1,), (1,)), ((), ())),
        precision=lax.Precision.HIGHEST, preferred_element_type=jnp.float32,
    )

    for j in range(1, n):
        norm_copy(lax.rem(z + j, n), z).start()

    def rows_copy(p, peer):
        return pltpu.make_async_remote_copy(
            src_ref=final.at[p, peer], dst_ref=recv.at[p, t], send_sem=asend.at[p], recv_sem=arecv.at[p],
            device_id={"ta": peer}, device_id_type=MESH,
        )

    def step(i, carry):
        p_final = i - (n - 2)
        p_out = p_final - 1

        for s in range(n - 1, 0, -1):
            p_right = i - (z - 1) - (n - 1 - s)

            @pl.when((z > 0) & (s > z) & (p_right >= 0) & (p_right < moms))
            def _():
                copy = rightward(rbuf, p_right, s)
                copy.wait_recv()
                for k in range(ppd):
                    rbuf[p_right, s * ppd + k] += parts[p_right, s * ppd + k]
                copy.start()

        for s in range(n - 1):
            p_left = i - (n - 2 - z) - s

            @pl.when((z < n - 1) & (s < z) & (p_left >= 0) & (p_left < moms))
            def _():
                copy = leftward(lbuf, p_left, s)
                copy.wait_recv()
                for k in range(ppd):
                    lbuf[p_left, s * ppd + k] += parts[p_left, s * ppd + k]
                copy.start()

        @pl.when((p_final >= 0) & (p_final < moms))
        def _():
            @pl.when(z > 0)
            def _():
                rightward(rbuf, p_final, z).wait_recv()
                for k in range(ppd):
                    parts[p_final, z * ppd + k] += rbuf[p_final, z * ppd + k]

            @pl.when(z < n - 1)
            def _():
                leftward(lbuf, p_final, z).wait_recv()
                for k in range(ppd):
                    parts[p_final, z * ppd + k] += lbuf[p_final, z * ppd + k]

            for k in range(ppd):
                value = parts[p_final, z * ppd + k] * scale
                for peer in range(nta):
                    final[p_final, peer, k] = value[peer * rows:(peer + 1) * rows]
            for j in range(1, nta):
                rows_copy(p_final, lax.rem(t + j, nta)).start()
            recv[p_final, t] = final[p_final, t]

        @pl.when((p_out >= 0) & (p_out < moms))
        def _():
            arrived = recv.at[p_out, pl.ds(0, nta - 1)]
            pltpu.make_async_copy(arrived, arrived, arecv.at[p_out]).wait()
            for source in range(nta):
                for k in range(ppd):
                    out_ref[p_out, k, :, source, :] = recv[p_out, source, k]

        return carry

    lax.fori_loop(0, moms + n - 1, step, 0)

    for j in range(1, n):
        norm_copy(lax.rem(z + j, n), lax.rem(z + j, n)).wait_recv()
    total = nbuf[0]
    for q in range(1, n):
        total = total + nbuf[q]
    norm_ref[...] = total[0:1] * inv_count
    for j in range(1, n):
        norm_copy(lax.rem(z + j, n), z).wait_send()

    def drain(p, carry):
        for s in range(n):
            @pl.when(s > z)
            def _():
                rightward(parts, p, s).wait_send()

            @pl.when(s < z)
            def _():
                leftward(parts, p, s).wait_send()
        sent = final.at[p, pl.ds(0, nta - 1)]
        pltpu.make_async_copy(sent, sent, asend.at[p]).wait()
        return carry

    lax.fori_loop(0, moms, drain, 0)


GV = 16


def pair_kernel(
    n, nta, scale, inv_count,
    order_ref, momenta_ref, ev_ref,
    out_ref, norm_ref,
    lown, lend, rown, rend, trig, vsend, vrecv, field, rbuf, ebuf, fin, recv, nbuf,
    vss, vrs, msend, mrecv, arecv, brecv, fsend, frecv, xsend, xrecv, nsend, nrecv,
):
    t, z = lax.axis_index("ta"), lax.axis_index("sa")
    moms, planes = momenta_ref.shape[1], ev_ref.shape[-1]
    half = NC * planes
    ng = BS // GV
    groups = NBLK * ng
    first_groups = groups // 2
    tile = 2 * GV
    wide = 2 * BS
    rows = BS // nta
    per = GV // rows
    hi = z // (n // 2)
    end_id = hi * (n - 1)
    mid_id = 1 + hi * (n - 3)
    other_id = n - 1 - z

    def blk(m, h):
        return m + h * (NBLK - 1 - 2 * m)

    def first(s, h):
        return blk(NBLK - 1 - lax.rem(s, 2), h) * ng + s // 2

    def second(s, h):
        return blk(NBLK - 1 - s // ng, h) * ng + lax.rem(s, ng)

    def at(start, size, step):
        return pl.ds(pl.multiple_of(start, step), size)

    row0, row1 = blk(0, hi) * wide, blk(1, hi) * wide
    row3 = blk(NBLK - 1, hi) * wide
    row2 = blk(NBLK - 2, hi) * wide
    far = (1 - hi) * 2 * wide
    rel3, rel2 = (1 - hi) * wide, hi * wide
    got0, got1 = hi * wide, (1 - hi) * wide

    barrier = pltpu.get_barrier_semaphore()
    for j in range(1, n):
        pl.semaphore_signal(barrier, inc=1, device_id={"sa": lax.rem(z + j, n)}, device_id_type=MESH)
    for j in range(1, nta):
        pl.semaphore_signal(barrier, inc=1, device_id={"ta": lax.rem(t + j, nta)}, device_id_type=MESH)

    def remote(src, dst, send_sem, recv_sem, peer):
        return pltpu.make_async_remote_copy(
            src_ref=src, dst_ref=dst, send_sem=send_sem, recv_sem=recv_sem,
            device_id={"sa": peer}, device_id_type=MESH,
        )

    def vector_copy(s):
        return remote(vsend.at[s], vrecv.at[s], vss.at[s], vrs.at[s], mid_id)

    def tile_copy(slot, group, rel):
        return remote(
            field.at[group, at(far + rel, tile, tile)], rbuf.at[group, at(rel, tile, tile)],
            msend.at[slot], mrecv.at[lax.rem(slot, first_groups)], other_id,
        )

    def a_copy(s, group, row, rel):
        return remote(
            field.at[group, at(row, wide, wide)], rbuf.at[group, at(rel, wide, wide)],
            msend.at[s], arecv.at[s - first_groups], other_id,
        )

    def b_copy(s, group, row, rel):
        return remote(
            field.at[group, at(row, wide, wide)], rbuf.at[group, at(rel, wide, wide)],
            msend.at[s], brecv.at[s - first_groups], other_id,
        )

    def forward_copy(slot, group):
        return remote(field.at[group, at(row0, wide, wide)], ebuf.at[group], fsend.at[slot], frecv.at[slot], end_id)

    def norm_copy(peer, slot):
        return remote(nbuf.at[slot], nbuf.at[slot], nsend.at[peer], nrecv.at[slot], peer)

    def rows_copy(group, peer):
        return pltpu.make_async_remote_copy(
            src_ref=fin.at[group, peer // per, :, lax.rem(peer, per)], dst_ref=recv.at[group, t],
            send_sem=xsend.at[group], recv_sem=xrecv.at[group],
            device_id={"ta": peer}, device_id_type=MESH,
        )

    def angles(slot, plane):
        site = lax.broadcasted_iota(jnp.int32, (1, planes), 1)
        for p in range(moms):
            phase_index = (
                momenta_ref[0, p] * lax.rem(site, LX)
                + momenta_ref[1, p] * lax.div(site, LX)
                + momenta_ref[2, p] * plane
            )
            angle = jnp.mod(phase_index, LX).astype(jnp.float32) * (full_turn / LX)
            trig[slot, 0, p:p + 1] = jnp.cos(angle)
            trig[slot, 1, p:p + 1] = jnp.sin(angle)

    def phased(load, slot, store):
        for c in range(NC):
            re, im = load(c), load(NC + c)
            for p in range(moms):
                cosine, sine = trig[slot, 0, p:p + 1], trig[slot, 1, p:p + 1]
                store(p, c, (re * cosine + im * sine).astype(jnp.bfloat16))
                store(p, NC + c, (im * cosine - re * sine).astype(jnp.bfloat16))

    def own_part(group, k):
        return lown[at(group * tile, GV, GV), k * planes:(k + 1) * planes].astype(jnp.float32)

    def own_right(group, base):
        def store(p, k, value):
            rown[base + p * GV:base + (p + 1) * GV, k * planes:(k + 1) * planes] = value
        phased(lambda k: own_part(group, k), 0, store)

    def times(a, b):
        return lax.dot_general(a, b, (((1,), (1,)), ((), ())), preferred_element_type=jnp.float32)

    def finish(group, value):
        value = value * scale
        fin[group] = value.reshape(ng, 2, per, rows, 128)
        for j in range(1, nta):
            rows_copy(group, lax.rem(t + j, nta)).start()
        recv[group, t] = fin[group, t // per, :, lax.rem(t, per)]

    lane = lax.broadcasted_iota(jnp.int32, (nta * rows, 128), 1) // GV

    def assemble(b):
        parts = []
        for g in range(ng):
            arrived = recv.at[b * ng + g, pl.ds(0, nta - 1)]
            pltpu.make_async_copy(arrived, arrived, xrecv.at[b * ng + g]).wait()
        for c in range(2):
            for g in range(ng):
                parts.append(recv[b * ng + g, :, c].reshape(nta * rows, 128))
        d = moms // 2
        while d:
            keep = (lane // d) % 2 == 0
            later = list(parts)
            for i in range(moms):
                if (i // d) % 2 == 0:
                    low, high = parts[i], parts[i + d]
                    later[i] = jnp.where(keep, low, pltpu.roll(high, d * GV, 1))
                    later[i + d] = jnp.where(keep, pltpu.roll(low, 128 - d * GV, 1), high)
            parts = later
            d //= 2
        for p in range(moms):
            for source in range(nta):
                out_ref[p, b, :, source, :] = parts[p][source * rows:(source + 1) * rows]

    def norms():
        squares = []
        for b in range(NBLK):
            total = jnp.zeros((BS, 128), jnp.float32)
            for k in range(2 * NC):
                for at_lane in range(0, planes, 128):
                    value = ev_ref[k, b, :, at_lane:at_lane + 128].astype(jnp.float32)
                    total = total + value * value
            squares.append(total)
        nbuf[z] = lax.dot_general(
            jnp.ones((8, 128), jnp.float32), jnp.concatenate(squares, axis=0), (((1,), (1,)), ((), ())),
            precision=lax.Precision.HIGHEST, preferred_element_type=jnp.float32,
        )
        for j in range(1, n):
            norm_copy(lax.rem(z + j, n), z).start()

    for b in range(NBLK):
        stored = order_ref[b]
        for k in range(2 * NC):
            value = ev_ref[k, stored]
            mirror = (k + NC) % (2 * NC)
            turned = value if k < NC else -value
            for g in range(ng):
                base = (b * ng + g) * tile
                lown[base:base + GV, k * planes:(k + 1) * planes] = value[g * GV:(g + 1) * GV]
                lown[base + GV:base + tile, mirror * planes:(mirror + 1) * planes] = turned[g * GV:(g + 1) * GV]

    @pl.when(lax.rem(z, n - 1) == 0)
    def _():
        def widen(s, group):
            vsend[s] = lown[at(group * tile, GV, GV), :].astype(jnp.float32)

        def widen_first(s, carry):
            widen(s, first(s, hi))
            return carry

        def widen_second(s, carry):
            widen(s, second(s, hi))
            return carry

        lax.fori_loop(0, first_groups, widen_first, 0)
        pl.semaphore_wait(barrier, n - 1 + nta - 1)
        for s in range(first_groups):
            vector_copy(s).start()
        lax.fori_loop(first_groups, groups, widen_second, 0)
        for s in range(first_groups, groups):
            vector_copy(s).start()
        angles(0, z)

        def own(i, carry):
            for q in range(2):
                own_right(2 * i + q, q * 128)
            value = times(lown[at(row0, wide, wide), :], rown[...])
            for q in range(2):
                field[2 * i + q, at(row0, wide, wide)] = value[:, q * 128:(q + 1) * 128]
            return carry

        lax.fori_loop(0, first_groups, own, 0)
        norms()

        def take(s, group):
            forward_copy(s, group).wait_recv()
            finish(group, field[group, at(row0, wide, wide)] + ebuf[group])

        def take_first(s, carry):
            take(s, first(s, 1 - hi))
            return carry

        def take_second(s, carry):
            take(s, second(s, 1 - hi))
            return carry

        lax.fori_loop(0, first_groups, take_first, 0)
        lax.fori_loop(first_groups, groups - ng, take_second, 0)

        def put(m, carry):
            assemble(blk(m, hi))
            return carry

        lax.fori_loop(0, NBLK - 1, put, 0)
        lax.fori_loop(groups - ng, groups, take_second, 0)
        assemble(blk(NBLK - 1, hi))

        def drain(s, carry):
            vector_copy(s).wait_send()
            return carry

        lax.fori_loop(0, groups, drain, 0)

    @pl.when(lax.rem(z, n - 1) != 0)
    def _():
        angles(0, z)
        angles(1, end_id)

        def own(i):
            pair = (first(i, hi), second(i + first_groups, hi))
            for q in range(2):
                own_right(pair[q], q * 128)
            value = times(lown[...], rown[...])
            for q in range(2):
                field[pair[q]] = value[:, q * 128:(q + 1) * 128]

        def arrive(s, group):
            vector_copy(s).wait_recv()
            base = group * tile
            for k in range(2 * NC):
                value = vrecv[s, :, k * planes:(k + 1) * planes]
                mirror = (k + NC) % (2 * NC)
                turned = value if k < NC else -value
                lend[at(base, GV, GV), k * planes:(k + 1) * planes] = value.astype(jnp.bfloat16)
                lend[at(base + GV, GV, GV), mirror * planes:(mirror + 1) * planes] = turned.astype(jnp.bfloat16)

            def store(p, k, value):
                rend[s, p * GV:(p + 1) * GV, k * planes:(k + 1) * planes] = value
            phased(lambda k: vrecv[s, :, k * planes:(k + 1) * planes], 1, store)

        def first_step(s, carry):
            own(s)

            @pl.when(s == 0)
            def _():
                pl.semaphore_wait(barrier, n - 1 + nta - 1)
                norms()

            group = first(s, hi)
            arrive(s, group)
            value = times(lend[at(far, 2 * wide, 2 * wide), :], rend[s])
            for u in range(2 * ng):
                came = 2 * (u % ng) + (1 - u // ng) + hi * (2 * (u // ng) - 1)

                @pl.when(came <= s)
                def _():
                    field[group, at(far + u * tile, tile, tile)] += value[u * tile:(u + 1) * tile]
                    tile_copy(s, group, u * tile).start()

            row = group * tile
            rel = row - far

            def earlier(i, carry):
                before = first(i, hi)
                field[before, at(row, tile, tile)] += times(lend[at(row, tile, tile), :], rend[i])
                tile_copy(i, before, rel).start()
                return carry

            lax.fori_loop(0, s, earlier, 0)
            return carry

        lax.fori_loop(0, first_groups, first_step, 0)

        def far_rows(s):
            group = second(s, hi)
            arrive(s, group)
            field[group, at(far, 2 * wide, 2 * wide)] += times(lend[at(far, 2 * wide, 2 * wide), :], rend[s])
            a_copy(s, group, row3, rel3).start()

            @pl.when(s >= first_groups + 2)
            def _():
                b_copy(s - 2, second(s - 2, hi), row2, rel2).start()

        def pass_on(slot, group):
            field[group, at(row0, wide, wide)] += rbuf[group, at(got0, wide, wide)]
            forward_copy(slot, group).start()

        def take_a(s):
            group = second(s, 1 - hi)
            a_copy(s, group, row0, got0).wait_recv()
            pass_on(s, group)

        def take_b(s):
            group = second(s, 1 - hi)
            b_copy(s, group, row1, got1).wait_recv()
            field[group, at(row1, wide, wide)] += rbuf[group, at(got1, wide, wide)]
            finish(group, field[group, at(row1, wide, wide)])

        def take_first(s, carry):
            group = first(s, 1 - hi)
            arrived = rbuf.at[group]
            pltpu.make_async_copy(arrived, arrived, mrecv.at[s]).wait()
            pass_on(s, group)
            field[group, at(row1, wide, wide)] += rbuf[group, at(got1, wide, wide)]
            return carry

        def second_step(s, carry):
            @pl.when(s == first_groups + 3)
            def _():
                lax.fori_loop(0, first_groups, take_first, 0)
                take_a(first_groups)

            far_rows(s)
            return carry

        lax.fori_loop(first_groups, groups - ng, second_step, 0)

        def third_step(s, carry):
            step = s - (groups - ng)
            take_a(s - 3)

            @pl.when(step >= 1)
            def _():
                take_b(s - 5)

            far_rows(s)
            group = second(s, hi)
            near = lend[at(row1, wide, wide), :]
            finish(group, field[group, at(row1, wide, wide)] + times(near, rend[s]))

            @pl.when(step < ng - 1)
            def _():
                late = step // 2

                def catch_up(q, carry):
                    odd = 2 * q + 1 - lax.rem(step, 2)
                    slot = late * (first_groups + q) + (1 - late) * odd
                    before = late * second(first_groups + q, hi) + (1 - late) * first(odd, hi)
                    field[before, at(row1, wide, wide)] += times(lend[at(row1, wide, wide), :], rend[slot])

                    @pl.when(late == 1)
                    def _():
                        finish(before, field[before, at(row1, wide, wide)])
                    return carry

                lax.fori_loop(0, ng, catch_up, 0)
            return carry

        lax.fori_loop(groups - ng, groups, third_step, 0)
        for s in (groups - 2, groups - 1):
            b_copy(s, second(s, hi), row2, rel2).start()

        def last_a(s, carry):
            take_a(s)
            return carry

        def last_b(s, carry):
            take_b(s)
            return carry

        lax.fori_loop(groups - 3, groups - 1, last_a, 0)
        lax.fori_loop(groups - 5, groups - ng, last_b, 0)
        lax.fori_loop(groups - 1, groups, last_a, 0)

        def put(m, carry):
            assemble(blk(m, hi))
            return carry

        lax.fori_loop(0, NBLK - 1, put, 0)
        lax.fori_loop(groups - ng, groups, last_b, 0)
        assemble(blk(NBLK - 1, hi))

        def drain(s, carry):
            sent = rbuf.at[s]
            pltpu.make_async_copy(sent, sent, msend.at[s]).wait()
            forward_copy(s, s).wait_send()
            return carry

        lax.fori_loop(0, groups, drain, 0)

    for j in range(1, n):
        norm_copy(lax.rem(z + j, n), lax.rem(z + j, n)).wait_recv()
    total = nbuf[0]
    for q in range(1, n):
        total = total + nbuf[q]
    norm_ref[...] = total[0:1] * inv_count
    for j in range(1, n):
        norm_copy(lax.rem(z + j, n), z).wait_send()

    def drain_rows(group, carry):
        sent = recv.at[group, pl.ds(0, nta - 1)]
        pltpu.make_async_copy(sent, sent, xsend.at[group]).wait()
        return carry

    lax.fori_loop(0, groups, drain_rows, 0)


def pair_scratch(n, nta, moms, nv, planes):
    f32, bf16 = jnp.float32, jnp.bfloat16
    deep = 2 * NC * planes
    ng = BS // GV
    groups = NBLK * ng
    rows = BS // nta
    dma = pltpu.SemaphoreType.DMA
    return [
        pltpu.VMEM((2 * nv, deep), bf16),
        pltpu.VMEM((2 * nv, deep), bf16),
        pltpu.VMEM((256, deep), bf16),
        pltpu.VMEM((groups, moms * GV, deep), bf16),
        pltpu.VMEM((2, 2, moms, planes), f32),
        pltpu.VMEM((groups, GV, deep), f32),
        pltpu.VMEM((groups, GV, deep), f32),
        pltpu.VMEM((groups, 2 * nv, 128), f32),
        pltpu.VMEM((groups, nv, 128), f32),
        pltpu.VMEM((groups, 2 * BS, 128), f32),
        pltpu.VMEM((groups, ng, 2, GV // rows, rows, 128), f32),
        pltpu.VMEM((groups, nta, 2, rows, 128), f32),
        pltpu.VMEM((n, 8, nv), f32),
        dma((groups,)), dma((groups,)), dma((groups,)), dma((groups // 2,)),
        dma((groups // 2,)), dma((groups // 2,)), dma((groups,)), dma((groups,)),
        dma((groups,)), dma((groups,)), dma((n,)), dma((n,)),
    ]


def line_scratch(n, nta, moms, nv, planes):
    f32 = jnp.float32
    ppd = NBLK * NBLK // n
    rows = BS // nta
    dma = pltpu.SemaphoreType.DMA
    return [
        pltpu.VMEM((nv, 2 * NC * planes), jnp.bfloat16),
        pltpu.VMEM((2 * nv, 2 * NC * planes), jnp.bfloat16),
        pltpu.VMEM((moms, NBLK * NBLK, BS, 2 * BS), f32),
        pltpu.VMEM((moms, NBLK * NBLK, BS, 2 * BS), f32),
        pltpu.VMEM((moms, NBLK * NBLK, BS, 2 * BS), f32),
        pltpu.VMEM((moms, nta, ppd, rows, 2 * BS), f32),
        pltpu.VMEM((moms, nta, ppd, rows, 2 * BS), f32),
        pltpu.VMEM((n, 8, nv), f32),
        dma((moms, n)), dma((moms, n)), dma((moms, n)), dma((moms, n)),
        dma((moms,)), dma((moms,)), dma((n,)), dma((n,)),
    ]


def body(eigenvectors, momenta, block_order):
    planes = eigenvectors.shape[-1]
    n, nta = lax.axis_size("sa"), lax.axis_size("ta")
    moms = momenta.shape[0]
    nv = eigenvectors.shape[1]
    ppd = NBLK * NBLK // n
    rows = BS // nta
    stored = eigenvectors.reshape(NBLK, BS, 2 * NC, planes).transpose(2, 0, 1, 3)
    count = 2 * NC * n * planes
    f32 = jnp.float32
    vmem = pl.BlockSpec(memory_space=pltpu.VMEM)
    smem = pl.BlockSpec(memory_space=pltpu.SMEM)
    paired = n == NBLK == 4 and moms * GV == 128 and rows % 8 == 0 and GV % rows == 0
    kernel, scratch = (pair_kernel, pair_scratch) if paired else (line_kernel, line_scratch)
    fields, norms = pl.pallas_call(
        functools.partial(kernel, n, nta, 1.0 / math.sqrt(count), 1.0 / count),
        out_shape=(
            jax.ShapeDtypeStruct((moms, ppd, rows, nta, 2 * BS), f32),
            jax.ShapeDtypeStruct((1, nv), f32),
        ),
        in_specs=[smem, smem, vmem],
        out_specs=(vmem, vmem),
        scratch_shapes=scratch(n, nta, moms, nv, planes),
        compiler_params=pltpu.CompilerParams(collective_id=0, has_side_effects=True, vmem_limit_bytes=48 * 1024 * 1024),
    )(block_order, momenta.T, stored)
    return fields, norms


def solution(mesh):
    return jax.shard_map(
        body,
        mesh=mesh,
        in_specs=(P("ta", None, None, None, "sa", None), P(), P()),
        out_specs=(P(None, "sa", "ta", None, None), P("ta", None)),
        check_vma=False,
    )
```

```python
import functools
import math

import jax
import jax.numpy as jnp
from jax import lax
from jax.experimental import pallas as pl
from jax.experimental.pallas import tpu as pltpu
from jax.sharding import PartitionSpec as P

NC = 3
BS = 64
NBLK = 4
LX = 96
MESH = pl.DeviceIdType.MESH

full_turn = 2.0 * math.pi


def line_kernel(
    n, nta, scale, inv_count,
    order_ref, momenta_ref, ev_ref,
    out_ref, norm_ref,
    left, right, parts, rbuf, lbuf, final, recv, nbuf,
    rsend, rrecv, lsend, lrecv, asend, arecv, nsend, nrecv,
):
    t, z = lax.axis_index("ta"), lax.axis_index("sa")
    moms, planes = momenta_ref.shape[1], ev_ref.shape[-1]
    ppd = NBLK * NBLK // n
    rows = BS // nta
    half = NC * planes

    barrier = pltpu.get_barrier_semaphore()
    for j in range(1, n):
        pl.semaphore_signal(barrier, inc=1, device_id={"sa": lax.rem(z + j, n)}, device_id_type=MESH)
    for j in range(1, nta):
        pl.semaphore_signal(barrier, inc=1, device_id={"ta": lax.rem(t + j, nta)}, device_id_type=MESH)

    for b in range(NBLK):
        stored = order_ref[b]
        for k in range(2 * NC):
            left[b * BS:(b + 1) * BS, k * planes:(k + 1) * planes] = ev_ref[k, stored]
    def norm_copy(peer, slot):
        return pltpu.make_async_remote_copy(
            src_ref=nbuf.at[slot], dst_ref=nbuf.at[slot], send_sem=nsend.at[peer], recv_sem=nrecv.at[slot],
            device_id={"sa": peer}, device_id_type=MESH,
        )

    def shard(ref, p, s):
        return ref.at[p, pl.ds(s * ppd, ppd)]

    def rightward(src, p, s):
        return pltpu.make_async_remote_copy(
            src_ref=shard(src, p, s), dst_ref=shard(rbuf, p, s), send_sem=rsend.at[p, s], recv_sem=rrecv.at[p, s],
            device_id={"sa": lax.rem(z + 1, n)}, device_id_type=MESH,
        )

    def leftward(src, p, s):
        return pltpu.make_async_remote_copy(
            src_ref=shard(src, p, s), dst_ref=shard(lbuf, p, s), send_sem=lsend.at[p, s], recv_sem=lrecv.at[p, s],
            device_id={"sa": lax.rem(z + n - 1, n)}, device_id_type=MESH,
        )

    def compute(p):
        site = lax.broadcasted_iota(jnp.int32, (1, planes), 1)
        phase_index = (
            momenta_ref[0, p] * lax.rem(site, LX)
            + momenta_ref[1, p] * lax.div(site, LX)
            + momenta_ref[2, p] * z
        )
        angles = jnp.mod(phase_index, LX).astype(jnp.float32) * (full_turn / LX)
        cosine, sine = jnp.cos(angles), jnp.sin(angles)
        for c in range(NC):
            lanes = slice(c * planes, (c + 1) * planes)
            upper = slice(half + c * planes, half + (c + 1) * planes)
            for b in range(NBLK):
                re = left[b * BS:(b + 1) * BS, lanes].astype(jnp.float32)
                im = left[b * BS:(b + 1) * BS, upper].astype(jnp.float32)
                phased_re = (re * cosine + im * sine).astype(jnp.bfloat16)
                phased_im = (im * cosine - re * sine).astype(jnp.bfloat16)
                first = slice(2 * b * BS, (2 * b + 1) * BS)
                second = slice((2 * b + 1) * BS, (2 * b + 2) * BS)
                right[first, lanes] = phased_re
                right[first, upper] = phased_im
                right[second, lanes] = phased_im
                right[second, upper] = -phased_re
        for pair in range(NBLK // 2):
            product = lax.dot_general(
                left[...], right[pair * 4 * BS:(pair + 1) * 4 * BS, :], (((1,), (1,)), ((), ())),
                preferred_element_type=jnp.float32,
            )
            for a in range(NBLK):
                for b in range(2):
                    parts[p, a * NBLK + 2 * pair + b] = product[a * BS:(a + 1) * BS, b * 2 * BS:(b + 1) * 2 * BS]

    def open_lines(slot):
        @pl.when(z == 0)
        def _():
            for s in range(n - 1, 0, -1):
                p = slot - (n - 1 - s)

                @pl.when((p >= 0) & (p < moms))
                def _():
                    rightward(parts, p, s).start()

        @pl.when(z == n - 1)
        def _():
            for s in range(n - 1):
                p = slot - s

                @pl.when((p >= 0) & (p < moms))
                def _():
                    leftward(parts, p, s).start()

    def compute_and_open(p, carry):
        compute(p)
        open_lines(p)
        return carry

    def only_open(slot, carry):
        open_lines(slot)
        return carry

    compute(0)
    pl.semaphore_wait(barrier, n - 1 + nta - 1)
    open_lines(0)
    lax.fori_loop(1, moms, compute_and_open, 0)
    lax.fori_loop(moms, moms + n - 2, only_open, 0)

    squares = []
    for b in range(NBLK):
        total = jnp.zeros((BS, 128), jnp.float32)
        for k in range(2 * NC):
            for lane in range(0, planes, 128):
                value = ev_ref[k, b, :, lane:lane + 128].astype(jnp.float32)
                total = total + value * value
        squares.append(total)
    nbuf[z] = lax.dot_general(
        jnp.ones((8, 128), jnp.float32), jnp.concatenate(squares, axis=0), (((1,), (1,)), ((), ())),
        precision=lax.Precision.HIGHEST, preferred_element_type=jnp.float32,
    )

    for j in range(1, n):
        norm_copy(lax.rem(z + j, n), z).start()

    def rows_copy(p, peer):
        return pltpu.make_async_remote_copy(
            src_ref=final.at[p, peer], dst_ref=recv.at[p, t], send_sem=asend.at[p], recv_sem=arecv.at[p],
            device_id={"ta": peer}, device_id_type=MESH,
        )

    def step(i, carry):
        p_final = i - (n - 2)
        p_out = p_final - 1

        for s in range(n - 1, 0, -1):
            p_right = i - (z - 1) - (n - 1 - s)

            @pl.when((z > 0) & (s > z) & (p_right >= 0) & (p_right < moms))
            def _():
                copy = rightward(rbuf, p_right, s)
                copy.wait_recv()
                for k in range(ppd):
                    rbuf[p_right, s * ppd + k] += parts[p_right, s * ppd + k]
                copy.start()

        for s in range(n - 1):
            p_left = i - (n - 2 - z) - s

            @pl.when((z < n - 1) & (s < z) & (p_left >= 0) & (p_left < moms))
            def _():
                copy = leftward(lbuf, p_left, s)
                copy.wait_recv()
                for k in range(ppd):
                    lbuf[p_left, s * ppd + k] += parts[p_left, s * ppd + k]
                copy.start()

        @pl.when((p_final >= 0) & (p_final < moms))
        def _():
            @pl.when(z > 0)
            def _():
                rightward(rbuf, p_final, z).wait_recv()
                for k in range(ppd):
                    parts[p_final, z * ppd + k] += rbuf[p_final, z * ppd + k]

            @pl.when(z < n - 1)
            def _():
                leftward(lbuf, p_final, z).wait_recv()
                for k in range(ppd):
                    parts[p_final, z * ppd + k] += lbuf[p_final, z * ppd + k]

            for k in range(ppd):
                value = parts[p_final, z * ppd + k] * scale
                for peer in range(nta):
                    final[p_final, peer, k] = value[peer * rows:(peer + 1) * rows]
            for j in range(1, nta):
                rows_copy(p_final, lax.rem(t + j, nta)).start()
            recv[p_final, t] = final[p_final, t]

        @pl.when((p_out >= 0) & (p_out < moms))
        def _():
            arrived = recv.at[p_out, pl.ds(0, nta - 1)]
            pltpu.make_async_copy(arrived, arrived, arecv.at[p_out]).wait()
            for source in range(nta):
                for k in range(ppd):
                    out_ref[p_out, k, :, source, :] = recv[p_out, source, k]

        return carry

    lax.fori_loop(0, moms + n - 1, step, 0)

    for j in range(1, n):
        norm_copy(lax.rem(z + j, n), lax.rem(z + j, n)).wait_recv()
    total = nbuf[0]
    for q in range(1, n):
        total = total + nbuf[q]
    norm_ref[...] = total[0:1] * inv_count
    for j in range(1, n):
        norm_copy(lax.rem(z + j, n), z).wait_send()

    def drain(p, carry):
        for s in range(n):
            @pl.when(s > z)
            def _():
                rightward(parts, p, s).wait_send()

            @pl.when(s < z)
            def _():
                leftward(parts, p, s).wait_send()
        sent = final.at[p, pl.ds(0, nta - 1)]
        pltpu.make_async_copy(sent, sent, asend.at[p]).wait()
        return carry

    lax.fori_loop(0, moms, drain, 0)


GV = 16


def pair_kernel(
    n, nta, scale, inv_count,
    order_ref, momenta_ref, ev_ref,
    out_ref, norm_ref,
    lown, lend, rown, rend, trig, vsend, vrecv, field, rbuf, ebuf, fin, recv, straight, late, nbuf,
    vss, vrs, msend, mrecv, arecv, brecv, fsend, frecv, xsend, xrecv, lsend, lrecv, nsend, nrecv, ready,
):
    t, z = lax.axis_index("ta"), lax.axis_index("sa")
    moms, planes = momenta_ref.shape[1], ev_ref.shape[-1]
    half = NC * planes
    ng = BS // GV
    groups = NBLK * ng
    first_groups = groups // 2
    tile = 2 * GV
    wide = 2 * BS
    rows = BS // nta
    per = GV // rows
    hi = z // (n // 2)
    end_id = hi * (n - 1)
    mid_id = 1 + hi * (n - 3)
    other_id = n - 1 - z

    def blk(m, h):
        return m + h * (NBLK - 1 - 2 * m)

    def first(s, h):
        return blk(NBLK - 1 - lax.rem(s, 2), h) * ng + s // 2

    def second(s, h):
        return blk(NBLK - 1 - s // ng, h) * ng + lax.rem(s, ng)

    def at(start, size, step):
        return pl.ds(pl.multiple_of(start, step), size)

    row0, row1 = blk(0, hi) * wide, blk(1, hi) * wide
    row3 = blk(NBLK - 1, hi) * wide
    row2 = blk(NBLK - 2, hi) * wide
    far = (1 - hi) * 2 * wide
    rel3, rel2 = (1 - hi) * wide, hi * wide
    got0, got1 = hi * wide, (1 - hi) * wide

    barrier = pltpu.get_barrier_semaphore()
    is_end = lax.rem(z, n - 1) == 0

    @pl.when(is_end)
    def _():
        pl.semaphore_signal(barrier, inc=1, device_id={"sa": mid_id}, device_id_type=MESH)

    @pl.when(jnp.logical_not(is_end))
    def _():
        for peer in (end_id, other_id):
            pl.semaphore_signal(barrier, inc=1, device_id={"sa": peer}, device_id_type=MESH)
        for j in range(1, nta):
            pl.semaphore_signal(barrier, inc=1, device_id={"ta": lax.rem(t + j, nta)}, device_id_type=MESH)

    def remote(src, dst, send_sem, recv_sem, peer):
        return pltpu.make_async_remote_copy(
            src_ref=src, dst_ref=dst, send_sem=send_sem, recv_sem=recv_sem,
            device_id={"sa": peer}, device_id_type=MESH,
        )

    def vector_copy(s):
        return remote(vsend.at[s], vrecv.at[s], vss.at[s], vrs.at[s], mid_id)

    def tile_copy(slot, group, rel):
        return remote(
            field.at[group, at(far + rel, tile, tile)], rbuf.at[group, at(rel, tile, tile)],
            msend.at[slot], mrecv.at[lax.rem(slot, first_groups)], other_id,
        )

    def a_copy(s, group, row, rel):
        return remote(
            field.at[group, at(row, wide, wide)], rbuf.at[group, at(rel, wide, wide)],
            msend.at[s], arecv.at[s - first_groups], other_id,
        )

    def b_copy(s, group, row, rel):
        return remote(
            field.at[group, at(row, wide, wide)], rbuf.at[group, at(rel, wide, wide)],
            msend.at[s], brecv.at[s - first_groups], other_id,
        )

    def forward_copy(slot, group):
        return remote(field.at[group, at(row0, wide, wide)], ebuf.at[group], fsend.at[slot], frecv.at[slot], end_id)

    def norm_copy(i, peer):
        return remote(nbuf.at[2 * i], nbuf.at[2 * i + 1], nsend.at[i], nrecv.at[i], peer)

    def straight_copy(i, part, row_peer, peer):
        return pltpu.make_async_remote_copy(
            src_ref=straight.at[i, part, row_peer // per, :, lax.rem(row_peer, per)], dst_ref=late.at[i, t],
            send_sem=lsend.at[i], recv_sem=lrecv.at[i],
            device_id={"ta": row_peer, "sa": peer}, device_id_type=MESH,
        )

    def rows_copy(group, peer):
        return pltpu.make_async_remote_copy(
            src_ref=fin.at[group, peer // per, :, lax.rem(peer, per)], dst_ref=recv.at[group, t],
            send_sem=xsend.at[group], recv_sem=xrecv.at[group],
            device_id={"ta": peer}, device_id_type=MESH,
        )

    def angles(slot, plane):
        site = lax.broadcasted_iota(jnp.int32, (1, planes), 1)
        for p in range(moms):
            phase_index = (
                momenta_ref[0, p] * lax.rem(site, LX)
                + momenta_ref[1, p] * lax.div(site, LX)
                + momenta_ref[2, p] * plane
            )
            angle = jnp.mod(phase_index, LX).astype(jnp.float32) * (full_turn / LX)
            trig[slot, 0, p:p + 1] = jnp.cos(angle)
            trig[slot, 1, p:p + 1] = jnp.sin(angle)

    def phased(load, slot, store):
        for c in range(NC):
            re, im = load(c), load(NC + c)
            for p in range(moms):
                cosine, sine = trig[slot, 0, p:p + 1], trig[slot, 1, p:p + 1]
                store(p, c, (re * cosine + im * sine).astype(jnp.bfloat16))
                store(p, NC + c, (im * cosine - re * sine).astype(jnp.bfloat16))

    def own_part(group, k):
        return lown[at(group * tile, GV, GV), k * planes:(k + 1) * planes].astype(jnp.float32)

    def own_right(group, base):
        def store(p, k, value):
            rown[base + p * GV:base + (p + 1) * GV, k * planes:(k + 1) * planes] = value
        phased(lambda k: own_part(group, k), 0, store)

    def times(a, b):
        return lax.dot_general(a, b, (((1,), (1,)), ((), ())), preferred_element_type=jnp.float32)

    def finish(group, value):
        value = value * scale
        fin[group] = value.reshape(ng, 2, per, rows, 128)
        for j in range(1, nta):
            rows_copy(group, lax.rem(t + j, nta)).start()
        recv[group, t] = fin[group, t // per, :, lax.rem(t, per)]

    lane = lax.broadcasted_iota(jnp.int32, (nta * rows, 128), 1) // GV

    def assemble(b, last):
        parts = []
        for g in range(ng):
            arrived = recv.at[b * ng + g, pl.ds(0, nta - 1)]
            pltpu.make_async_copy(arrived, arrived, xrecv.at[b * ng + g]).wait()
            if last:
                pltpu.make_async_copy(late.at[g], late.at[g], lrecv.at[g]).wait()
        for c in range(2):
            for g in range(ng):
                part = recv[b * ng + g, :, c].reshape(nta * rows, 128)
                if last:
                    part = part + late[g, :, c].reshape(nta * rows, 128)
                parts.append(part)
        d = moms // 2
        while d:
            keep = (lane // d) % 2 == 0
            later = list(parts)
            for i in range(moms):
                if (i // d) % 2 == 0:
                    low, high = parts[i], parts[i + d]
                    later[i] = jnp.where(keep, low, pltpu.roll(high, d * GV, 1))
                    later[i + d] = jnp.where(keep, pltpu.roll(low, 128 - d * GV, 1), high)
            parts = later
            d //= 2
        for p in range(moms):
            for source in range(nta):
                out_ref[p, b, :, source, :] = parts[p][source * rows:(source + 1) * rows]

    def norms():
        squares = []
        for b in range(NBLK):
            total = jnp.zeros((BS, 128), jnp.float32)
            for k in range(2 * NC):
                for at_lane in range(0, planes, 128):
                    value = ev_ref[k, b, :, at_lane:at_lane + 128].astype(jnp.float32)
                    total = total + value * value
            squares.append(total)
        nbuf[0] = lax.dot_general(
            jnp.ones((8, 128), jnp.float32), jnp.concatenate(squares, axis=0), (((1,), (1,)), ((), ())),
            precision=lax.Precision.HIGHEST, preferred_element_type=jnp.float32,
        )

    for b in range(NBLK):
        stored = order_ref[b]
        for k in range(2 * NC):
            value = ev_ref[k, stored]
            mirror = (k + NC) % (2 * NC)
            turned = value if k < NC else -value
            for g in range(ng):
                base = (b * ng + g) * tile
                lown[base:base + GV, k * planes:(k + 1) * planes] = value[g * GV:(g + 1) * GV]
                lown[base + GV:base + tile, mirror * planes:(mirror + 1) * planes] = turned[g * GV:(g + 1) * GV]

    @pl.when(is_end)
    def _():
        def widen(s, group):
            vsend[s] = lown[at(group * tile, GV, GV), :].astype(jnp.float32)

        def widen_first(s, carry):
            widen(s, first(s, hi))
            return carry

        def widen_second(s, carry):
            widen(s, second(s, hi))
            return carry

        lax.fori_loop(0, first_groups, widen_first, 0)
        pl.semaphore_wait(barrier, 1)
        for s in range(ng):
            vector_copy(s).start()
        norms()
        norm_copy(0, mid_id).start()
        for s in range(ng, first_groups):
            vector_copy(s).start()
        lax.fori_loop(first_groups, groups, widen_second, 0)
        for s in range(first_groups, groups):
            vector_copy(s).start()
        angles(0, z)

        def own(i, carry):
            for q in range(2):
                own_right(2 * i + q, q * 128)
            value = times(lown[at(row0, wide, wide), :], rown[...])
            for q in range(2):
                field[2 * i + q, at(row0, wide, wide)] = value[:, q * 128:(q + 1) * 128]
            return carry

        lax.fori_loop(0, first_groups, own, 0)

        def take(s, group):
            forward_copy(s, group).wait_recv()
            finish(group, field[group, at(row0, wide, wide)] + ebuf[group])

        def take_first(s, carry):
            take(s, first(s, 1 - hi))
            return carry

        def take_second(s, carry):
            take(s, second(s, 1 - hi))
            return carry

        lax.fori_loop(0, first_groups, take_first, 0)
        lax.fori_loop(groups - ng, groups, take_second, 0)

        def put(m, carry):
            assemble(blk(m, hi), False)
            return carry

        lax.fori_loop(0, 2, put, 0)
        lax.fori_loop(first_groups, groups - ng, take_second, 0)
        lax.fori_loop(2, NBLK - 1, put, 0)
        norm_copy(2, end_id).wait_recv()
        norm_ref[...] = nbuf[5, 0:1] * inv_count
        assemble(blk(NBLK - 1, hi), True)
        norm_copy(0, mid_id).wait_send()

        def drain(s, carry):
            vector_copy(s).wait_send()
            return carry

        lax.fori_loop(0, groups, drain, 0)

    @pl.when(jnp.logical_not(is_end))
    def _():
        angles(0, z)
        angles(1, end_id)

        def own(i):
            pair = (first(i, hi), second(i + first_groups, hi))
            for q in range(2):
                own_right(pair[q], q * 128)
            value = times(lown[...], rown[...])
            for q in range(2):
                field[pair[q]] = value[:, q * 128:(q + 1) * 128]

        def arrive(s, group):
            vector_copy(s).wait_recv()
            base = group * tile
            for k in range(2 * NC):
                value = vrecv[s, :, k * planes:(k + 1) * planes]
                mirror = (k + NC) % (2 * NC)
                turned = value if k < NC else -value
                lend[at(base, GV, GV), k * planes:(k + 1) * planes] = value.astype(jnp.bfloat16)
                lend[at(base + GV, GV, GV), mirror * planes:(mirror + 1) * planes] = turned.astype(jnp.bfloat16)

            def store(p, k, value):
                rend[s, p * GV:(p + 1) * GV, k * planes:(k + 1) * planes] = value
            phased(lambda k: vrecv[s, :, k * planes:(k + 1) * planes], 1, store)

        def first_step(s, carry):
            own(s)

            @pl.when(s == 0)
            def _():
                pl.semaphore_wait(barrier, nta + 1)
                for j in range(1, nta):
                    pl.semaphore_signal(ready, inc=1, device_id={"ta": lax.rem(t + j, nta)}, device_id_type=MESH)
                norms()
                pl.semaphore_wait(ready, nta - 1)

            group = first(s, hi)

            @pl.when(lax.rem(s, 2) == 0)
            def _():
                forward_copy(groups - ng + s // 2, group).start()

            arrive(s, group)
            value = times(lend[at(far, 2 * wide, 2 * wide), :], rend[s])
            for u in range(2 * ng):
                came = 2 * (u % ng) + (1 - u // ng) + hi * (2 * (u // ng) - 1)

                @pl.when(came <= s)
                def _():
                    field[group, at(far + u * tile, tile, tile)] += value[u * tile:(u + 1) * tile]
                    tile_copy(s, group, u * tile).start()

            row = group * tile
            rel = row - far

            def earlier(i, carry):
                before = first(i, hi)
                field[before, at(row, tile, tile)] += times(lend[at(row, tile, tile), :], rend[i])
                tile_copy(i, before, rel).start()
                return carry

            lax.fori_loop(0, s, earlier, 0)
            return carry

        lax.fori_loop(0, first_groups, first_step, 0)

        def far_rows(s):
            group = second(s, hi)
            arrive(s, group)
            field[group, at(far, 2 * wide, 2 * wide)] += times(lend[at(far, 2 * wide, 2 * wide), :], rend[s])
            return group

        def send_b(s):
            b_copy(s, second(s, hi), row2, rel2).start()

        def send_straight(i, part, group, row, peer):
            value = field[group, at(row, wide, wide)] * scale
            straight[i, part] = value.reshape(ng, 2, per, rows, 128)
            for j in range(nta):
                straight_copy(i, part, lax.rem(t + j, nta), peer).start()

        def straight_a(s):
            send_straight(s - (groups - ng), 0, second(s, hi), row3, n - 1 - end_id)

        def straight_b(s):
            send_straight(s - (groups - ng), 1, second(s, hi), row2, other_id)

        def pass_on(slot, group):
            field[group, at(row0, wide, wide)] += rbuf[group, at(got0, wide, wide)]
            forward_copy(slot, group).start()

        def take_a(s):
            group = second(s, 1 - hi)
            a_copy(s, group, row0, got0).wait_recv()
            pass_on(s, group)

        def take_b(s):
            group = second(s, 1 - hi)
            b_copy(s, group, row1, got1).wait_recv()
            field[group, at(row1, wide, wide)] += rbuf[group, at(got1, wide, wide)]
            finish(group, field[group, at(row1, wide, wide)])

        def take_first(s, carry):
            group = first(s, 1 - hi)
            arrived = rbuf.at[group]
            pltpu.make_async_copy(arrived, arrived, mrecv.at[s]).wait()
            pass_on(s, group)
            field[group, at(row1, wide, wide)] += rbuf[group, at(got1, wide, wide)]
            return carry

        def last_a(s, carry):
            take_a(s)
            return carry

        def second_step(s, carry):
            @pl.when(s == first_groups + 2)
            def _():
                lax.fori_loop(0, first_groups, take_first, 0)

            @pl.when(s == first_groups + 3)
            def _():
                lax.fori_loop(first_groups, first_groups + 2, last_a, 0)

            @pl.when(s == first_groups)
            def _():
                norm_copy(0, mid_id).wait_recv()
                nbuf[2] = nbuf[0] + nbuf[1]
                norm_copy(1, other_id).start()

            group = far_rows(s)
            a_copy(s, group, row3, rel3).start()

            @pl.when(s >= first_groups + 2)
            def _():
                send_b(s - 2)
            return carry

        lax.fori_loop(first_groups, groups - ng, second_step, 0)

        def third_step(s, carry):
            step = s - (groups - ng)

            @pl.when(step == 0)
            def _():
                norm_copy(1, other_id).wait_recv()
                total = nbuf[2] + nbuf[3]
                nbuf[4] = total
                norm_ref[...] = total[0:1] * inv_count
                norm_copy(2, end_id).start()

            @pl.when(step < 2)
            def _():
                take_a(s - 2)

            @pl.when(step >= 2)
            def _():
                take_b(s - 6)

            group = far_rows(s)
            straight_a(s)

            @pl.when(step < 2)
            def _():
                send_b(s - 2)

            @pl.when(step >= 2)
            def _():
                straight_b(s - 2)
            near = lend[at(row1, wide, wide), :]
            finish(group, field[group, at(row1, wide, wide)] + times(near, rend[s]))

            @pl.when(step < ng - 1)
            def _():
                later = (2 - step) // 2

                def catch_up(q, carry):
                    odd = 2 * q + 2 - step
                    slot = later * (first_groups + q) + (1 - later) * odd
                    before = later * second(first_groups + q, hi) + (1 - later) * first(odd, hi)
                    field[before, at(row1, wide, wide)] += times(lend[at(row1, wide, wide), :], rend[slot])

                    @pl.when(step != 1)
                    def _():
                        finish(before, field[before, at(row1, wide, wide)])
                    return carry

                lax.fori_loop(0, ng, catch_up, 0)
            return carry

        lax.fori_loop(groups - ng, groups, third_step, 0)
        straight_b(groups - 2)
        straight_b(groups - 1)
        take_b(groups - 6)
        take_b(groups - 5)

        def put(m, carry):
            assemble(blk(m, hi), False)
            return carry

        lax.fori_loop(0, NBLK - 1, put, 0)
        assemble(blk(NBLK - 1, hi), True)
        norm_copy(1, other_id).wait_send()
        norm_copy(2, end_id).wait_send()

        def drain(s, carry):
            forward_copy(s, s).wait_send()
            return carry

        def drain_sums(s, carry):
            sent = rbuf.at[s]
            pltpu.make_async_copy(sent, sent, msend.at[s]).wait()
            return carry

        def drain_straight(i, carry):
            sent = straight.at[i]
            pltpu.make_async_copy(sent, sent, lsend.at[i]).wait()
            return carry

        lax.fori_loop(0, groups, drain, 0)
        lax.fori_loop(0, groups - ng, drain_sums, 0)
        lax.fori_loop(0, ng, drain_straight, 0)

    def drain_rows(group, carry):
        sent = recv.at[group, pl.ds(0, nta - 1)]
        pltpu.make_async_copy(sent, sent, xsend.at[group]).wait()
        return carry

    lax.fori_loop(0, groups, drain_rows, 0)


def pair_scratch(n, nta, moms, nv, planes):
    f32, bf16 = jnp.float32, jnp.bfloat16
    deep = 2 * NC * planes
    ng = BS // GV
    groups = NBLK * ng
    rows = BS // nta
    dma = pltpu.SemaphoreType.DMA
    return [
        pltpu.VMEM((2 * nv, deep), bf16),
        pltpu.VMEM((2 * nv, deep), bf16),
        pltpu.VMEM((256, deep), bf16),
        pltpu.VMEM((groups, moms * GV, deep), bf16),
        pltpu.VMEM((2, 2, moms, planes), f32),
        pltpu.VMEM((groups, GV, deep), f32),
        pltpu.VMEM((groups, GV, deep), f32),
        pltpu.VMEM((groups, 2 * nv, 128), f32),
        pltpu.VMEM((groups, nv, 128), f32),
        pltpu.VMEM((groups, 2 * BS, 128), f32),
        pltpu.VMEM((groups, ng, 2, GV // rows, rows, 128), f32),
        pltpu.VMEM((groups, nta, 2, rows, 128), f32),
        pltpu.VMEM((ng, 2, ng, 2, GV // rows, rows, 128), f32),
        pltpu.VMEM((ng, nta, 2, rows, 128), f32),
        pltpu.VMEM((6, 8, nv), f32),
        dma((groups,)), dma((groups,)), dma((groups,)), dma((groups // 2,)),
        dma((groups // 2,)), dma((groups // 2,)), dma((groups,)), dma((groups,)),
        dma((groups,)), dma((groups,)), dma((ng,)), dma((ng,)), dma((3,)), dma((3,)),
        pltpu.SemaphoreType.REGULAR,
    ]


def line_scratch(n, nta, moms, nv, planes):
    f32 = jnp.float32
    ppd = NBLK * NBLK // n
    rows = BS // nta
    dma = pltpu.SemaphoreType.DMA
    return [
        pltpu.VMEM((nv, 2 * NC * planes), jnp.bfloat16),
        pltpu.VMEM((2 * nv, 2 * NC * planes), jnp.bfloat16),
        pltpu.VMEM((moms, NBLK * NBLK, BS, 2 * BS), f32),
        pltpu.VMEM((moms, NBLK * NBLK, BS, 2 * BS), f32),
        pltpu.VMEM((moms, NBLK * NBLK, BS, 2 * BS), f32),
        pltpu.VMEM((moms, nta, ppd, rows, 2 * BS), f32),
        pltpu.VMEM((moms, nta, ppd, rows, 2 * BS), f32),
        pltpu.VMEM((n, 8, nv), f32),
        dma((moms, n)), dma((moms, n)), dma((moms, n)), dma((moms, n)),
        dma((moms,)), dma((moms,)), dma((n,)), dma((n,)),
    ]


def body(eigenvectors, momenta, block_order):
    planes = eigenvectors.shape[-1]
    n, nta = lax.axis_size("sa"), lax.axis_size("ta")
    moms = momenta.shape[0]
    nv = eigenvectors.shape[1]
    ppd = NBLK * NBLK // n
    rows = BS // nta
    stored = eigenvectors.reshape(NBLK, BS, 2 * NC, planes).transpose(2, 0, 1, 3)
    count = 2 * NC * n * planes
    f32 = jnp.float32
    vmem = pl.BlockSpec(memory_space=pltpu.VMEM)
    smem = pl.BlockSpec(memory_space=pltpu.SMEM)
    paired = n == NBLK == 4 and moms * GV == 128 and rows % 8 == 0 and GV % rows == 0
    kernel, scratch = (pair_kernel, pair_scratch) if paired else (line_kernel, line_scratch)
    fields, norms = pl.pallas_call(
        functools.partial(kernel, n, nta, 1.0 / math.sqrt(count), 1.0 / count),
        out_shape=(
            jax.ShapeDtypeStruct((moms, ppd, rows, nta, 2 * BS), f32),
            jax.ShapeDtypeStruct((1, nv), f32),
        ),
        in_specs=[smem, smem, vmem],
        out_specs=(vmem, vmem),
        scratch_shapes=scratch(n, nta, moms, nv, planes),
        compiler_params=pltpu.CompilerParams(collective_id=0, has_side_effects=True, vmem_limit_bytes=48 * 1024 * 1024),
    )(block_order, momenta.T, stored)
    return fields, norms


def solution(mesh):
    return jax.shard_map(
        body,
        mesh=mesh,
        in_specs=(P("ta", None, None, None, "sa", None), P(), P()),
        out_specs=(P(None, "sa", "ta", None, None), P("ta", None)),
        check_vma=False,
    )
```

```python
import functools
import math

import jax
import jax.numpy as jnp
from jax import lax
from jax.experimental import pallas as pl
from jax.experimental.pallas import tpu as pltpu
from jax.sharding import PartitionSpec as P

NC = 3
BS = 64
NBLK = 4
LX = 96
MESH = pl.DeviceIdType.MESH

full_turn = 2.0 * math.pi


def line_kernel(
    n, nta, scale, inv_count,
    order_ref, momenta_ref, ev_ref,
    out_ref, norm_ref,
    left, right, parts, rbuf, lbuf, final, recv, nbuf,
    rsend, rrecv, lsend, lrecv, asend, arecv, nsend, nrecv,
):
    t, z = lax.axis_index("ta"), lax.axis_index("sa")
    moms, planes = momenta_ref.shape[1], ev_ref.shape[-1]
    ppd = NBLK * NBLK // n
    rows = BS // nta
    half = NC * planes

    barrier = pltpu.get_barrier_semaphore()
    for j in range(1, n):
        pl.semaphore_signal(barrier, inc=1, device_id={"sa": lax.rem(z + j, n)}, device_id_type=MESH)
    for j in range(1, nta):
        pl.semaphore_signal(barrier, inc=1, device_id={"ta": lax.rem(t + j, nta)}, device_id_type=MESH)

    for b in range(NBLK):
        stored = order_ref[b]
        for k in range(2 * NC):
            left[b * BS:(b + 1) * BS, k * planes:(k + 1) * planes] = ev_ref[k, stored]
    def norm_copy(peer, slot):
        return pltpu.make_async_remote_copy(
            src_ref=nbuf.at[slot], dst_ref=nbuf.at[slot], send_sem=nsend.at[peer], recv_sem=nrecv.at[slot],
            device_id={"sa": peer}, device_id_type=MESH,
        )

    def shard(ref, p, s):
        return ref.at[p, pl.ds(s * ppd, ppd)]

    def rightward(src, p, s):
        return pltpu.make_async_remote_copy(
            src_ref=shard(src, p, s), dst_ref=shard(rbuf, p, s), send_sem=rsend.at[p, s], recv_sem=rrecv.at[p, s],
            device_id={"sa": lax.rem(z + 1, n)}, device_id_type=MESH,
        )

    def leftward(src, p, s):
        return pltpu.make_async_remote_copy(
            src_ref=shard(src, p, s), dst_ref=shard(lbuf, p, s), send_sem=lsend.at[p, s], recv_sem=lrecv.at[p, s],
            device_id={"sa": lax.rem(z + n - 1, n)}, device_id_type=MESH,
        )

    def compute(p):
        site = lax.broadcasted_iota(jnp.int32, (1, planes), 1)
        phase_index = (
            momenta_ref[0, p] * lax.rem(site, LX)
            + momenta_ref[1, p] * lax.div(site, LX)
            + momenta_ref[2, p] * z
        )
        angles = jnp.mod(phase_index, LX).astype(jnp.float32) * (full_turn / LX)
        cosine, sine = jnp.cos(angles), jnp.sin(angles)
        for c in range(NC):
            lanes = slice(c * planes, (c + 1) * planes)
            upper = slice(half + c * planes, half + (c + 1) * planes)
            for b in range(NBLK):
                re = left[b * BS:(b + 1) * BS, lanes].astype(jnp.float32)
                im = left[b * BS:(b + 1) * BS, upper].astype(jnp.float32)
                phased_re = (re * cosine + im * sine).astype(jnp.bfloat16)
                phased_im = (im * cosine - re * sine).astype(jnp.bfloat16)
                first = slice(2 * b * BS, (2 * b + 1) * BS)
                second = slice((2 * b + 1) * BS, (2 * b + 2) * BS)
                right[first, lanes] = phased_re
                right[first, upper] = phased_im
                right[second, lanes] = phased_im
                right[second, upper] = -phased_re
        for pair in range(NBLK // 2):
            product = lax.dot_general(
                left[...], right[pair * 4 * BS:(pair + 1) * 4 * BS, :], (((1,), (1,)), ((), ())),
                preferred_element_type=jnp.float32,
            )
            for a in range(NBLK):
                for b in range(2):
                    parts[p, a * NBLK + 2 * pair + b] = product[a * BS:(a + 1) * BS, b * 2 * BS:(b + 1) * 2 * BS]

    def open_lines(slot):
        @pl.when(z == 0)
        def _():
            for s in range(n - 1, 0, -1):
                p = slot - (n - 1 - s)

                @pl.when((p >= 0) & (p < moms))
                def _():
                    rightward(parts, p, s).start()

        @pl.when(z == n - 1)
        def _():
            for s in range(n - 1):
                p = slot - s

                @pl.when((p >= 0) & (p < moms))
                def _():
                    leftward(parts, p, s).start()

    def compute_and_open(p, carry):
        compute(p)
        open_lines(p)
        return carry

    def only_open(slot, carry):
        open_lines(slot)
        return carry

    compute(0)
    pl.semaphore_wait(barrier, n - 1 + nta - 1)
    open_lines(0)
    lax.fori_loop(1, moms, compute_and_open, 0)
    lax.fori_loop(moms, moms + n - 2, only_open, 0)

    squares = []
    for b in range(NBLK):
        total = jnp.zeros((BS, 128), jnp.float32)
        for k in range(2 * NC):
            for lane in range(0, planes, 128):
                value = ev_ref[k, b, :, lane:lane + 128].astype(jnp.float32)
                total = total + value * value
        squares.append(total)
    nbuf[z] = lax.dot_general(
        jnp.ones((8, 128), jnp.float32), jnp.concatenate(squares, axis=0), (((1,), (1,)), ((), ())),
        precision=lax.Precision.HIGHEST, preferred_element_type=jnp.float32,
    )

    for j in range(1, n):
        norm_copy(lax.rem(z + j, n), z).start()

    def rows_copy(p, peer):
        return pltpu.make_async_remote_copy(
            src_ref=final.at[p, peer], dst_ref=recv.at[p, t], send_sem=asend.at[p], recv_sem=arecv.at[p],
            device_id={"ta": peer}, device_id_type=MESH,
        )

    def step(i, carry):
        p_final = i - (n - 2)
        p_out = p_final - 1

        for s in range(n - 1, 0, -1):
            p_right = i - (z - 1) - (n - 1 - s)

            @pl.when((z > 0) & (s > z) & (p_right >= 0) & (p_right < moms))
            def _():
                copy = rightward(rbuf, p_right, s)
                copy.wait_recv()
                for k in range(ppd):
                    rbuf[p_right, s * ppd + k] += parts[p_right, s * ppd + k]
                copy.start()

        for s in range(n - 1):
            p_left = i - (n - 2 - z) - s

            @pl.when((z < n - 1) & (s < z) & (p_left >= 0) & (p_left < moms))
            def _():
                copy = leftward(lbuf, p_left, s)
                copy.wait_recv()
                for k in range(ppd):
                    lbuf[p_left, s * ppd + k] += parts[p_left, s * ppd + k]
                copy.start()

        @pl.when((p_final >= 0) & (p_final < moms))
        def _():
            @pl.when(z > 0)
            def _():
                rightward(rbuf, p_final, z).wait_recv()
                for k in range(ppd):
                    parts[p_final, z * ppd + k] += rbuf[p_final, z * ppd + k]

            @pl.when(z < n - 1)
            def _():
                leftward(lbuf, p_final, z).wait_recv()
                for k in range(ppd):
                    parts[p_final, z * ppd + k] += lbuf[p_final, z * ppd + k]

            for k in range(ppd):
                value = parts[p_final, z * ppd + k] * scale
                for peer in range(nta):
                    final[p_final, peer, k] = value[peer * rows:(peer + 1) * rows]
            for j in range(1, nta):
                rows_copy(p_final, lax.rem(t + j, nta)).start()
            recv[p_final, t] = final[p_final, t]

        @pl.when((p_out >= 0) & (p_out < moms))
        def _():
            arrived = recv.at[p_out, pl.ds(0, nta - 1)]
            pltpu.make_async_copy(arrived, arrived, arecv.at[p_out]).wait()
            for source in range(nta):
                for k in range(ppd):
                    out_ref[p_out, k, :, source, :] = recv[p_out, source, k]

        return carry

    lax.fori_loop(0, moms + n - 1, step, 0)

    for j in range(1, n):
        norm_copy(lax.rem(z + j, n), lax.rem(z + j, n)).wait_recv()
    total = nbuf[0]
    for q in range(1, n):
        total = total + nbuf[q]
    norm_ref[...] = total[0:1] * inv_count
    for j in range(1, n):
        norm_copy(lax.rem(z + j, n), z).wait_send()

    def drain(p, carry):
        for s in range(n):
            @pl.when(s > z)
            def _():
                rightward(parts, p, s).wait_send()

            @pl.when(s < z)
            def _():
                leftward(parts, p, s).wait_send()
        sent = final.at[p, pl.ds(0, nta - 1)]
        pltpu.make_async_copy(sent, sent, asend.at[p]).wait()
        return carry

    lax.fori_loop(0, moms, drain, 0)


GV = 16


def pair_kernel(
    n, nta, scale, inv_count,
    order_ref, momenta_ref, ev_ref,
    out_ref, norm_ref,
    lown, lend, rown, rend, trig, vsend, vrecv, field, rbuf, ebuf, fin, recv, straight, late, nbuf,
    vss, vrs, msend, mrecv, arecv, brecv, fsend, frecv, xsend, xrecv, lsend, lrecv, nsend, nrecv, ready,
):
    t, z = lax.axis_index("ta"), lax.axis_index("sa")
    moms, planes = momenta_ref.shape[1], ev_ref.shape[-1]
    half = NC * planes
    ng = BS // GV
    groups = NBLK * ng
    first_groups = groups // 2
    tile = 2 * GV
    wide = 2 * BS
    rows = BS // nta
    per = GV // rows
    hi = z // (n // 2)
    end_id = hi * (n - 1)
    mid_id = 1 + hi * (n - 3)
    other_id = n - 1 - z

    def blk(m, h):
        return m + h * (NBLK - 1 - 2 * m)

    def first(s, h):
        return blk(NBLK - 1 - lax.rem(s, 2), h) * ng + s // 2

    def second(s, h):
        return blk(NBLK - 1 - s // ng, h) * ng + lax.rem(s, ng)

    def at(start, size, step):
        return pl.ds(pl.multiple_of(start, step), size)

    row0, row1 = blk(0, hi) * wide, blk(1, hi) * wide
    row3 = blk(NBLK - 1, hi) * wide
    row2 = blk(NBLK - 2, hi) * wide
    far = (1 - hi) * 2 * wide
    rel3, rel2 = (1 - hi) * wide, hi * wide
    got0, got1 = hi * wide, (1 - hi) * wide

    barrier = pltpu.get_barrier_semaphore()
    is_end = lax.rem(z, n - 1) == 0

    @pl.when(is_end)
    def _():
        pl.semaphore_signal(barrier, inc=1, device_id={"sa": mid_id}, device_id_type=MESH)

    @pl.when(jnp.logical_not(is_end))
    def _():
        for peer in (end_id, other_id):
            pl.semaphore_signal(barrier, inc=1, device_id={"sa": peer}, device_id_type=MESH)
        for j in range(1, nta):
            pl.semaphore_signal(barrier, inc=1, device_id={"ta": lax.rem(t + j, nta)}, device_id_type=MESH)

    def remote(src, dst, send_sem, recv_sem, peer):
        return pltpu.make_async_remote_copy(
            src_ref=src, dst_ref=dst, send_sem=send_sem, recv_sem=recv_sem,
            device_id={"sa": peer}, device_id_type=MESH,
        )

    def vector_copy(s):
        return remote(vsend.at[s], vrecv.at[s], vss.at[s], vrs.at[s], mid_id)

    def tile_copy(slot, group, rel):
        return remote(
            field.at[group, at(far + rel, tile, tile)], rbuf.at[group, at(rel, tile, tile)],
            msend.at[slot], mrecv.at[lax.rem(slot, first_groups)], other_id,
        )

    def a_copy(s, group, row, rel):
        return remote(
            field.at[group, at(row, wide, wide)], rbuf.at[group, at(rel, wide, wide)],
            msend.at[s], arecv.at[s - first_groups], other_id,
        )

    def b_copy(s, group, row, rel):
        return remote(
            field.at[group, at(row, wide, wide)], rbuf.at[group, at(rel, wide, wide)],
            msend.at[s], brecv.at[s - first_groups], other_id,
        )

    def forward_copy(slot, group):
        return remote(field.at[group, at(row0, wide, wide)], ebuf.at[group], fsend.at[slot], frecv.at[slot], end_id)

    def norm_copy(i, peer):
        return remote(nbuf.at[2 * i], nbuf.at[2 * i + 1], nsend.at[i], nrecv.at[i], peer)

    def straight_copy(i, part, row_peer, peer):
        return pltpu.make_async_remote_copy(
            src_ref=straight.at[i, part, row_peer], dst_ref=late.at[i, t],
            send_sem=lsend.at[i], recv_sem=lrecv.at[i],
            device_id={"ta": row_peer, "sa": peer}, device_id_type=MESH,
        )

    def rows_copy(group, peer):
        return pltpu.make_async_remote_copy(
            src_ref=fin.at[group, peer], dst_ref=recv.at[group, t],
            send_sem=xsend.at[group], recv_sem=xrecv.at[group],
            device_id={"ta": peer}, device_id_type=MESH,
        )

    def angles(slot, plane):
        site = lax.broadcasted_iota(jnp.int32, (1, planes), 1)
        for p in range(moms):
            phase_index = (
                momenta_ref[0, p] * lax.rem(site, LX)
                + momenta_ref[1, p] * lax.div(site, LX)
                + momenta_ref[2, p] * plane
            )
            angle = jnp.mod(phase_index, LX).astype(jnp.float32) * (full_turn / LX)
            trig[slot, 0, p:p + 1] = jnp.cos(angle)
            trig[slot, 1, p:p + 1] = jnp.sin(angle)

    def phased(load, slot, store):
        for c in range(NC):
            re, im = load(c), load(NC + c)
            for p in range(moms):
                cosine, sine = trig[slot, 0, p:p + 1], trig[slot, 1, p:p + 1]
                store(p, c, (re * cosine + im * sine).astype(jnp.bfloat16))
                store(p, NC + c, (im * cosine - re * sine).astype(jnp.bfloat16))

    def own_part(group, k):
        return lown[at(group * tile, GV, GV), k * planes:(k + 1) * planes].astype(jnp.float32)

    def own_right(group, base):
        def store(p, k, value):
            rown[base + p * GV:base + (p + 1) * GV, k * planes:(k + 1) * planes] = value
        phased(lambda k: own_part(group, k), 0, store)

    def times(a, b):
        return lax.dot_general(a, b, (((1,), (1,)), ((), ())), preferred_element_type=jnp.float32)

    def split(value, ref):
        for peer in range(nta):
            for c in range(2):
                base = peer // per * tile + c * GV + peer % per * rows
                ref[peer, c] = value[base:base + rows]

    def finish(group, value):
        split(value * scale, fin.at[group])
        for j in range(1, nta):
            rows_copy(group, lax.rem(t + j, nta)).start()
        recv[group, t] = fin[group, t]

    lane = lax.broadcasted_iota(jnp.int32, (nta * rows, 128), 1) // GV

    def assemble(b, last):
        parts = []
        for g in range(ng):
            arrived = recv.at[b * ng + g, pl.ds(0, nta - 1)]
            pltpu.make_async_copy(arrived, arrived, xrecv.at[b * ng + g]).wait()
            if last:
                pltpu.make_async_copy(late.at[g], late.at[g], lrecv.at[g]).wait()
        for c in range(2):
            for g in range(ng):
                part = recv[b * ng + g, :, c].reshape(nta * rows, 128)
                if last:
                    part = part + late[g, :, c].reshape(nta * rows, 128)
                parts.append(part)
        d = moms // 2
        while d:
            keep = (lane // d) % 2 == 0
            later = list(parts)
            for i in range(moms):
                if (i // d) % 2 == 0:
                    low, high = parts[i], parts[i + d]
                    later[i] = jnp.where(keep, low, pltpu.roll(high, d * GV, 1))
                    later[i + d] = jnp.where(keep, pltpu.roll(low, 128 - d * GV, 1), high)
            parts = later
            d //= 2
        for p in range(moms):
            for source in range(nta):
                out_ref[p, b, :, source, :] = parts[p][source * rows:(source + 1) * rows]

    def drain_rows(group, carry):
        sent = recv.at[group, pl.ds(0, nta - 1)]
        pltpu.make_async_copy(sent, sent, xsend.at[group]).wait()
        return carry

    def norms():
        squares = []
        for b in range(NBLK):
            total = jnp.zeros((BS, 128), jnp.float32)
            for k in range(2 * NC):
                for at_lane in range(0, planes, 128):
                    value = ev_ref[k, b, :, at_lane:at_lane + 128].astype(jnp.float32)
                    total = total + value * value
            squares.append(total)
        nbuf[0] = lax.dot_general(
            jnp.ones((8, 128), jnp.float32), jnp.concatenate(squares, axis=0), (((1,), (1,)), ((), ())),
            precision=lax.Precision.HIGHEST, preferred_element_type=jnp.float32,
        )

    def build():
        for b in range(NBLK):
            stored = order_ref[b]
            for k in range(2 * NC):
                value = ev_ref[k, stored]
                mirror = (k + NC) % (2 * NC)
                turned = value if k < NC else -value
                for g in range(ng):
                    base = (b * ng + g) * tile
                    lown[base:base + GV, k * planes:(k + 1) * planes] = value[g * GV:(g + 1) * GV]
                    lown[base + GV:base + tile, mirror * planes:(mirror + 1) * planes] = turned[g * GV:(g + 1) * GV]

    @pl.when(is_end)
    def _():
        def widen(s, group):
            stored = order_ref[group // ng]
            for k in range(2 * NC):
                value = ev_ref[k, stored, at(lax.rem(group, ng) * GV, GV, GV), :]
                vsend[s, :, k * planes:(k + 1) * planes] = value.astype(jnp.float32)

        def widen_first(s, carry):
            widen(s, first(s, hi))
            return carry

        def widen_second(s, carry):
            widen(s, second(s, hi))
            return carry

        lax.fori_loop(0, ng, widen_first, 0)
        pl.semaphore_wait(barrier, 1)
        for s in range(ng):
            vector_copy(s).start()
        lax.fori_loop(ng, first_groups, widen_first, 0)
        norms()
        norm_copy(0, mid_id).start()
        for s in range(ng, first_groups):
            vector_copy(s).start()
        lax.fori_loop(first_groups, groups, widen_second, 0)
        for s in range(first_groups, groups):
            vector_copy(s).start()
        angles(0, z)
        build()

        def own(i, carry):
            for q in range(2):
                own_right(2 * i + q, q * 128)
            value = times(lown[at(row0, wide, wide), :], rown[...])
            for q in range(2):
                field[2 * i + q, at(row0, wide, wide)] = value[:, q * 128:(q + 1) * 128]
            return carry

        lax.fori_loop(0, first_groups, own, 0)

        def take(s, group):
            forward_copy(s, group).wait_recv()
            finish(group, field[group, at(row0, wide, wide)] + ebuf[group])

        def take_first(s, carry):
            take(s, first(s, 1 - hi))
            return carry

        def take_second(s, carry):
            take(s, second(s, 1 - hi))
            return carry

        lax.fori_loop(0, first_groups, take_first, 0)
        lax.fori_loop(groups - ng, groups, take_second, 0)

        def put(m, carry):
            assemble(blk(m, hi), False)
            return carry

        lax.fori_loop(0, 2, put, 0)
        lax.fori_loop(first_groups, groups - ng, take_second, 0)
        lax.fori_loop(2, NBLK - 1, put, 0)
        norm_copy(2, end_id).wait_recv()
        norm_ref[...] = nbuf[5, 0:1] * inv_count
        norm_copy(0, mid_id).wait_send()

        def drain(s, carry):
            vector_copy(s).wait_send()
            return carry

        lax.fori_loop(0, groups, drain, 0)
        lax.fori_loop(0, groups, drain_rows, 0)
        assemble(blk(NBLK - 1, hi), True)

    @pl.when(jnp.logical_not(is_end))
    def _():
        build()
        angles(0, z)
        angles(1, end_id)

        def own(i):
            pair = (first(i, hi), second(i + first_groups, hi))
            for q in range(2):
                own_right(pair[q], q * 128)
            value = times(lown[...], rown[...])
            for q in range(2):
                field[pair[q]] = value[:, q * 128:(q + 1) * 128]

        def arrive(s, group, rows_too=True):
            vector_copy(s).wait_recv()
            base = group * tile
            for k in range(2 * NC if rows_too else 0):
                value = vrecv[s, :, k * planes:(k + 1) * planes]
                mirror = (k + NC) % (2 * NC)
                turned = value if k < NC else -value
                lend[at(base, GV, GV), k * planes:(k + 1) * planes] = value.astype(jnp.bfloat16)
                lend[at(base + GV, GV, GV), mirror * planes:(mirror + 1) * planes] = turned.astype(jnp.bfloat16)

            def store(p, k, value):
                rend[s, p * GV:(p + 1) * GV, k * planes:(k + 1) * planes] = value
            phased(lambda k: vrecv[s, :, k * planes:(k + 1) * planes], 1, store)

        def first_step(s, carry):
            own(s)

            @pl.when(s == 0)
            def _():
                pl.semaphore_wait(barrier, nta + 1)
                for j in range(1, nta):
                    pl.semaphore_signal(ready, inc=1, device_id={"ta": lax.rem(t + j, nta)}, device_id_type=MESH)
                norms()
                pl.semaphore_wait(ready, nta - 1)

            group = first(s, hi)

            @pl.when(lax.rem(s, 2) == 0)
            def _():
                forward_copy(groups - ng + s // 2, group).start()

            arrive(s, group)
            value = times(lend[at(far, 2 * wide, 2 * wide), :], rend[s])
            for u in range(2 * ng):
                came = 2 * (u % ng) + (1 - u // ng) + hi * (2 * (u // ng) - 1)

                @pl.when(came <= s)
                def _():
                    field[group, at(far + u * tile, tile, tile)] += value[u * tile:(u + 1) * tile]
                    tile_copy(s, group, u * tile).start()

            row = group * tile
            rel = row - far

            def earlier(i, carry):
                before = first(i, hi)
                field[before, at(row, tile, tile)] += times(lend[at(row, tile, tile), :], rend[i])
                tile_copy(i, before, rel).start()
                return carry

            lax.fori_loop(0, s, earlier, 0)
            return carry

        lax.fori_loop(0, first_groups, first_step, 0)

        def far_rows(s, rows_too):
            group = second(s, hi)
            arrive(s, group, rows_too)
            field[group, at(far, 2 * wide, 2 * wide)] += times(lend[at(far, 2 * wide, 2 * wide), :], rend[s])
            return group

        def send_b(s):
            b_copy(s, second(s, hi), row2, rel2).start()

        def send_straight(i, part, group, row, peer):
            split(field[group, at(row, wide, wide)] * scale, straight.at[i, part])
            for j in range(nta):
                straight_copy(i, part, lax.rem(t + j, nta), peer).start()

        def straight_a(s):
            send_straight(s - (groups - ng), 0, second(s, hi), row3, n - 1 - end_id)

        def straight_b(s):
            send_straight(s - (groups - ng), 1, second(s, hi), row2, other_id)

        def pass_on(slot, group):
            field[group, at(row0, wide, wide)] += rbuf[group, at(got0, wide, wide)]
            forward_copy(slot, group).start()

        def take_a(s):
            group = second(s, 1 - hi)
            a_copy(s, group, row0, got0).wait_recv()
            pass_on(s, group)

        def take_b(s):
            group = second(s, 1 - hi)
            b_copy(s, group, row1, got1).wait_recv()
            field[group, at(row1, wide, wide)] += rbuf[group, at(got1, wide, wide)]
            finish(group, field[group, at(row1, wide, wide)])

        def take_first(s, carry):
            group = first(s, 1 - hi)
            arrived = rbuf.at[group]
            pltpu.make_async_copy(arrived, arrived, mrecv.at[s]).wait()
            pass_on(s, group)
            field[group, at(row1, wide, wide)] += rbuf[group, at(got1, wide, wide)]
            return carry

        def last_a(s, carry):
            take_a(s)
            return carry

        def second_step(s, carry):
            @pl.when(s == first_groups + 2)
            def _():
                lax.fori_loop(0, first_groups, take_first, 0)

            @pl.when(s == first_groups + 3)
            def _():
                lax.fori_loop(first_groups, first_groups + 2, last_a, 0)

            @pl.when(s == first_groups)
            def _():
                norm_copy(0, mid_id).wait_recv()
                nbuf[2] = nbuf[0] + nbuf[1]
                norm_copy(1, other_id).start()

            group = far_rows(s, True)
            a_copy(s, group, row3, rel3).start()

            send_b(s)
            return carry

        lax.fori_loop(first_groups, groups - ng, second_step, 0)

        def third_step(s, carry):
            step = s - (groups - ng)

            @pl.when(step == 0)
            def _():
                norm_copy(1, other_id).wait_recv()
                total = nbuf[2] + nbuf[3]
                nbuf[4] = total
                norm_ref[...] = total[0:1] * inv_count
                norm_copy(2, end_id).start()

            @pl.when(step < 2)
            def _():
                take_a(s - 2)

            @pl.when(step >= 2)
            def _():
                take_b(s - 6)

            group = far_rows(s, False)
            straight_a(s)

            straight_b(s)
            near = lend[at(row1, wide, wide), :]
            finish(group, field[group, at(row1, wide, wide)] + times(near, rend[s]))

            @pl.when(step < ng - 1)
            def _():
                later = (2 - step) // 2

                def catch_up(q, carry):
                    odd = 2 * q + 2 - step
                    slot = later * (first_groups + q) + (1 - later) * odd
                    before = later * second(first_groups + q, hi) + (1 - later) * first(odd, hi)
                    field[before, at(row1, wide, wide)] += times(lend[at(row1, wide, wide), :], rend[slot])

                    @pl.when(step != 1)
                    def _():
                        finish(before, field[before, at(row1, wide, wide)])
                    return carry

                lax.fori_loop(0, ng, catch_up, 0)
            return carry

        lax.fori_loop(groups - ng, groups, third_step, 0)
        take_b(groups - 6)
        take_b(groups - 5)

        def put(m, carry):
            assemble(blk(m, hi), False)
            return carry

        lax.fori_loop(0, NBLK - 1, put, 0)
        norm_copy(1, other_id).wait_send()
        norm_copy(2, end_id).wait_send()

        def drain(s, carry):
            forward_copy(s, s).wait_send()
            return carry

        def drain_sums(s, carry):
            sent = rbuf.at[s]
            pltpu.make_async_copy(sent, sent, msend.at[s]).wait()
            return carry

        def drain_straight(i, carry):
            sent = straight.at[i]
            pltpu.make_async_copy(sent, sent, lsend.at[i]).wait()
            return carry

        lax.fori_loop(0, groups, drain, 0)
        lax.fori_loop(0, groups - ng, drain_sums, 0)
        lax.fori_loop(0, groups, drain_rows, 0)
        lax.fori_loop(0, ng, drain_straight, 0)
        assemble(blk(NBLK - 1, hi), True)


def pair_scratch(n, nta, moms, nv, planes):
    f32, bf16 = jnp.float32, jnp.bfloat16
    deep = 2 * NC * planes
    ng = BS // GV
    groups = NBLK * ng
    rows = BS // nta
    dma = pltpu.SemaphoreType.DMA
    return [
        pltpu.VMEM((2 * nv, deep), bf16),
        pltpu.VMEM((2 * nv, deep), bf16),
        pltpu.VMEM((256, deep), bf16),
        pltpu.VMEM((groups, moms * GV, deep), bf16),
        pltpu.VMEM((2, 2, moms, planes), f32),
        pltpu.VMEM((groups, GV, deep), f32),
        pltpu.VMEM((groups, GV, deep), f32),
        pltpu.VMEM((groups, 2 * nv, 128), f32),
        pltpu.VMEM((groups, nv, 128), f32),
        pltpu.VMEM((groups, 2 * BS, 128), f32),
        pltpu.VMEM((groups, nta, 2, rows, 128), f32),
        pltpu.VMEM((groups, nta, 2, rows, 128), f32),
        pltpu.VMEM((ng, 2, nta, 2, rows, 128), f32),
        pltpu.VMEM((ng, nta, 2, rows, 128), f32),
        pltpu.VMEM((6, 8, nv), f32),
        dma((groups,)), dma((groups,)), dma((groups,)), dma((groups // 2,)),
        dma((groups // 2,)), dma((groups // 2,)), dma((groups,)), dma((groups,)),
        dma((groups,)), dma((groups,)), dma((ng,)), dma((ng,)), dma((3,)), dma((3,)),
        pltpu.SemaphoreType.REGULAR,
    ]


def line_scratch(n, nta, moms, nv, planes):
    f32 = jnp.float32
    ppd = NBLK * NBLK // n
    rows = BS // nta
    dma = pltpu.SemaphoreType.DMA
    return [
        pltpu.VMEM((nv, 2 * NC * planes), jnp.bfloat16),
        pltpu.VMEM((2 * nv, 2 * NC * planes), jnp.bfloat16),
        pltpu.VMEM((moms, NBLK * NBLK, BS, 2 * BS), f32),
        pltpu.VMEM((moms, NBLK * NBLK, BS, 2 * BS), f32),
        pltpu.VMEM((moms, NBLK * NBLK, BS, 2 * BS), f32),
        pltpu.VMEM((moms, nta, ppd, rows, 2 * BS), f32),
        pltpu.VMEM((moms, nta, ppd, rows, 2 * BS), f32),
        pltpu.VMEM((n, 8, nv), f32),
        dma((moms, n)), dma((moms, n)), dma((moms, n)), dma((moms, n)),
        dma((moms,)), dma((moms,)), dma((n,)), dma((n,)),
    ]


def body(eigenvectors, momenta, block_order):
    planes = eigenvectors.shape[-1]
    n, nta = lax.axis_size("sa"), lax.axis_size("ta")
    moms = momenta.shape[0]
    nv = eigenvectors.shape[1]
    ppd = NBLK * NBLK // n
    rows = BS // nta
    stored = eigenvectors.reshape(NBLK, BS, 2 * NC, planes).transpose(2, 0, 1, 3)
    count = 2 * NC * n * planes
    f32 = jnp.float32
    vmem = pl.BlockSpec(memory_space=pltpu.VMEM)
    smem = pl.BlockSpec(memory_space=pltpu.SMEM)
    paired = n == NBLK == 4 and moms * GV == 128 and rows % 8 == 0 and GV % rows == 0
    kernel, scratch = (pair_kernel, pair_scratch) if paired else (line_kernel, line_scratch)
    fields, norms = pl.pallas_call(
        functools.partial(kernel, n, nta, 1.0 / math.sqrt(count), 1.0 / count),
        out_shape=(
            jax.ShapeDtypeStruct((moms, ppd, rows, nta, 2 * BS), f32),
            jax.ShapeDtypeStruct((1, nv), f32),
        ),
        in_specs=[smem, smem, vmem],
        out_specs=(vmem, vmem),
        scratch_shapes=scratch(n, nta, moms, nv, planes),
        compiler_params=pltpu.CompilerParams(collective_id=0, has_side_effects=True, vmem_limit_bytes=48 * 1024 * 1024),
    )(block_order, momenta.T, stored)
    return fields, norms


def solution(mesh):
    return jax.shard_map(
        body,
        mesh=mesh,
        in_specs=(P("ta", None, None, None, "sa", None), P(), P()),
        out_specs=(P(None, "sa", "ta", None, None), P("ta", None)),
        check_vma=False,
    )
```

```python
import functools
import math

import jax
import jax.numpy as jnp
from jax import lax
from jax.experimental import pallas as pl
from jax.experimental.pallas import tpu as pltpu
from jax.sharding import PartitionSpec as P

NC = 3
BS = 64
NBLK = 4
LX = 96
MESH = pl.DeviceIdType.MESH

full_turn = 2.0 * math.pi


def line_kernel(
    n, nta, scale, inv_count,
    order_ref, momenta_ref, ev_ref,
    out_ref, norm_ref,
    left, right, parts, rbuf, lbuf, final, recv, nbuf,
    rsend, rrecv, lsend, lrecv, asend, arecv, nsend, nrecv,
):
    t, z = lax.axis_index("ta"), lax.axis_index("sa")
    moms, planes = momenta_ref.shape[1], ev_ref.shape[-1]
    ppd = NBLK * NBLK // n
    rows = BS // nta
    half = NC * planes

    barrier = pltpu.get_barrier_semaphore()
    for j in range(1, n):
        pl.semaphore_signal(barrier, inc=1, device_id={"sa": lax.rem(z + j, n)}, device_id_type=MESH)
    for j in range(1, nta):
        pl.semaphore_signal(barrier, inc=1, device_id={"ta": lax.rem(t + j, nta)}, device_id_type=MESH)

    for b in range(NBLK):
        stored = order_ref[b]
        for k in range(2 * NC):
            left[b * BS:(b + 1) * BS, k * planes:(k + 1) * planes] = ev_ref[k, stored]
    def norm_copy(peer, slot):
        return pltpu.make_async_remote_copy(
            src_ref=nbuf.at[slot], dst_ref=nbuf.at[slot], send_sem=nsend.at[peer], recv_sem=nrecv.at[slot],
            device_id={"sa": peer}, device_id_type=MESH,
        )

    def shard(ref, p, s):
        return ref.at[p, pl.ds(s * ppd, ppd)]

    def rightward(src, p, s):
        return pltpu.make_async_remote_copy(
            src_ref=shard(src, p, s), dst_ref=shard(rbuf, p, s), send_sem=rsend.at[p, s], recv_sem=rrecv.at[p, s],
            device_id={"sa": lax.rem(z + 1, n)}, device_id_type=MESH,
        )

    def leftward(src, p, s):
        return pltpu.make_async_remote_copy(
            src_ref=shard(src, p, s), dst_ref=shard(lbuf, p, s), send_sem=lsend.at[p, s], recv_sem=lrecv.at[p, s],
            device_id={"sa": lax.rem(z + n - 1, n)}, device_id_type=MESH,
        )

    def compute(p):
        site = lax.broadcasted_iota(jnp.int32, (1, planes), 1)
        phase_index = (
            momenta_ref[0, p] * lax.rem(site, LX)
            + momenta_ref[1, p] * lax.div(site, LX)
            + momenta_ref[2, p] * z
        )
        angles = jnp.mod(phase_index, LX).astype(jnp.float32) * (full_turn / LX)
        cosine, sine = jnp.cos(angles), jnp.sin(angles)
        for c in range(NC):
            lanes = slice(c * planes, (c + 1) * planes)
            upper = slice(half + c * planes, half + (c + 1) * planes)
            for b in range(NBLK):
                re = left[b * BS:(b + 1) * BS, lanes].astype(jnp.float32)
                im = left[b * BS:(b + 1) * BS, upper].astype(jnp.float32)
                phased_re = (re * cosine + im * sine).astype(jnp.bfloat16)
                phased_im = (im * cosine - re * sine).astype(jnp.bfloat16)
                first = slice(2 * b * BS, (2 * b + 1) * BS)
                second = slice((2 * b + 1) * BS, (2 * b + 2) * BS)
                right[first, lanes] = phased_re
                right[first, upper] = phased_im
                right[second, lanes] = phased_im
                right[second, upper] = -phased_re
        for pair in range(NBLK // 2):
            product = lax.dot_general(
                left[...], right[pair * 4 * BS:(pair + 1) * 4 * BS, :], (((1,), (1,)), ((), ())),
                preferred_element_type=jnp.float32,
            )
            for a in range(NBLK):
                for b in range(2):
                    parts[p, a * NBLK + 2 * pair + b] = product[a * BS:(a + 1) * BS, b * 2 * BS:(b + 1) * 2 * BS]

    def open_lines(slot):
        @pl.when(z == 0)
        def _():
            for s in range(n - 1, 0, -1):
                p = slot - (n - 1 - s)

                @pl.when((p >= 0) & (p < moms))
                def _():
                    rightward(parts, p, s).start()

        @pl.when(z == n - 1)
        def _():
            for s in range(n - 1):
                p = slot - s

                @pl.when((p >= 0) & (p < moms))
                def _():
                    leftward(parts, p, s).start()

    def compute_and_open(p, carry):
        compute(p)
        open_lines(p)
        return carry

    def only_open(slot, carry):
        open_lines(slot)
        return carry

    compute(0)
    pl.semaphore_wait(barrier, n - 1 + nta - 1)
    open_lines(0)
    lax.fori_loop(1, moms, compute_and_open, 0)
    lax.fori_loop(moms, moms + n - 2, only_open, 0)

    squares = []
    for b in range(NBLK):
        total = jnp.zeros((BS, 128), jnp.float32)
        for k in range(2 * NC):
            for lane in range(0, planes, 128):
                value = ev_ref[k, b, :, lane:lane + 128].astype(jnp.float32)
                total = total + value * value
        squares.append(total)
    nbuf[z] = lax.dot_general(
        jnp.ones((8, 128), jnp.float32), jnp.concatenate(squares, axis=0), (((1,), (1,)), ((), ())),
        precision=lax.Precision.HIGHEST, preferred_element_type=jnp.float32,
    )

    for j in range(1, n):
        norm_copy(lax.rem(z + j, n), z).start()

    def rows_copy(p, peer):
        return pltpu.make_async_remote_copy(
            src_ref=final.at[p, peer], dst_ref=recv.at[p, t], send_sem=asend.at[p], recv_sem=arecv.at[p],
            device_id={"ta": peer}, device_id_type=MESH,
        )

    def step(i, carry):
        p_final = i - (n - 2)
        p_out = p_final - 1

        for s in range(n - 1, 0, -1):
            p_right = i - (z - 1) - (n - 1 - s)

            @pl.when((z > 0) & (s > z) & (p_right >= 0) & (p_right < moms))
            def _():
                copy = rightward(rbuf, p_right, s)
                copy.wait_recv()
                for k in range(ppd):
                    rbuf[p_right, s * ppd + k] += parts[p_right, s * ppd + k]
                copy.start()

        for s in range(n - 1):
            p_left = i - (n - 2 - z) - s

            @pl.when((z < n - 1) & (s < z) & (p_left >= 0) & (p_left < moms))
            def _():
                copy = leftward(lbuf, p_left, s)
                copy.wait_recv()
                for k in range(ppd):
                    lbuf[p_left, s * ppd + k] += parts[p_left, s * ppd + k]
                copy.start()

        @pl.when((p_final >= 0) & (p_final < moms))
        def _():
            @pl.when(z > 0)
            def _():
                rightward(rbuf, p_final, z).wait_recv()
                for k in range(ppd):
                    parts[p_final, z * ppd + k] += rbuf[p_final, z * ppd + k]

            @pl.when(z < n - 1)
            def _():
                leftward(lbuf, p_final, z).wait_recv()
                for k in range(ppd):
                    parts[p_final, z * ppd + k] += lbuf[p_final, z * ppd + k]

            for k in range(ppd):
                value = parts[p_final, z * ppd + k] * scale
                for peer in range(nta):
                    final[p_final, peer, k] = value[peer * rows:(peer + 1) * rows]
            for j in range(1, nta):
                rows_copy(p_final, lax.rem(t + j, nta)).start()
            recv[p_final, t] = final[p_final, t]

        @pl.when((p_out >= 0) & (p_out < moms))
        def _():
            arrived = recv.at[p_out, pl.ds(0, nta - 1)]
            pltpu.make_async_copy(arrived, arrived, arecv.at[p_out]).wait()
            for source in range(nta):
                for k in range(ppd):
                    out_ref[p_out, k, :, source, :] = recv[p_out, source, k]

        return carry

    lax.fori_loop(0, moms + n - 1, step, 0)

    for j in range(1, n):
        norm_copy(lax.rem(z + j, n), lax.rem(z + j, n)).wait_recv()
    total = nbuf[0]
    for q in range(1, n):
        total = total + nbuf[q]
    norm_ref[...] = total[0:1] * inv_count
    for j in range(1, n):
        norm_copy(lax.rem(z + j, n), z).wait_send()

    def drain(p, carry):
        for s in range(n):
            @pl.when(s > z)
            def _():
                rightward(parts, p, s).wait_send()

            @pl.when(s < z)
            def _():
                leftward(parts, p, s).wait_send()
        sent = final.at[p, pl.ds(0, nta - 1)]
        pltpu.make_async_copy(sent, sent, asend.at[p]).wait()
        return carry

    lax.fori_loop(0, moms, drain, 0)


GV = 16


def pair_kernel(
    n, nta, scale, inv_count,
    order_ref, momenta_ref, ev_ref,
    out_ref, norm_ref,
    lown, lend, rown, rend, trig, vsend, vrecv, field, rbuf, ebuf, fin, recv, straight, late, nbuf,
    vss, vrs, msend, mrecv, arecv, brecv, fsend, frecv, xsend, xrecv, lsend, lrecv, nsend, nrecv, ready,
):
    t, z = lax.axis_index("ta"), lax.axis_index("sa")
    moms, planes = momenta_ref.shape[1], ev_ref.shape[-1]
    half = NC * planes
    ng = BS // GV
    groups = NBLK * ng
    first_groups = groups // 2
    tile = 2 * GV
    wide = 2 * BS
    rows = BS // nta
    per = GV // rows
    hi = z // (n // 2)
    end_id = hi * (n - 1)
    mid_id = 1 + hi * (n - 3)
    other_id = n - 1 - z

    def blk(m, h):
        return m + h * (NBLK - 1 - 2 * m)

    def first(s, h):
        return blk(NBLK - 1 - lax.rem(s, 2), h) * ng + s // 2

    def second(s, h):
        return blk(NBLK - 1 - s // ng, h) * ng + lax.rem(s, ng)

    def at(start, size, step):
        return pl.ds(pl.multiple_of(start, step), size)

    row0, row1 = blk(0, hi) * wide, blk(1, hi) * wide
    row3 = blk(NBLK - 1, hi) * wide
    row2 = blk(NBLK - 2, hi) * wide
    far = (1 - hi) * 2 * wide
    rel3, rel2 = (1 - hi) * wide, hi * wide
    got0, got1 = hi * wide, (1 - hi) * wide

    barrier = pltpu.get_barrier_semaphore()
    is_end = lax.rem(z, n - 1) == 0

    @pl.when(is_end)
    def _():
        pl.semaphore_signal(barrier, inc=1, device_id={"sa": mid_id}, device_id_type=MESH)

    @pl.when(jnp.logical_not(is_end))
    def _():
        for peer in (end_id, other_id):
            pl.semaphore_signal(barrier, inc=1, device_id={"sa": peer}, device_id_type=MESH)
        for j in range(1, nta):
            pl.semaphore_signal(barrier, inc=1, device_id={"ta": lax.rem(t + j, nta)}, device_id_type=MESH)

    def remote(src, dst, send_sem, recv_sem, peer):
        return pltpu.make_async_remote_copy(
            src_ref=src, dst_ref=dst, send_sem=send_sem, recv_sem=recv_sem,
            device_id={"sa": peer}, device_id_type=MESH,
        )

    def vector_copy(s):
        return remote(vsend.at[s], vrecv.at[s], vss.at[s], vrs.at[s], mid_id)

    def tile_copy(slot, group, rel):
        return remote(
            field.at[group, at(far + rel, tile, tile)], rbuf.at[group, at(rel, tile, tile)],
            msend.at[slot], mrecv.at[lax.rem(slot, first_groups)], other_id,
        )

    def a_copy(s, group, row, rel):
        return remote(
            field.at[group, at(row, wide, wide)], rbuf.at[group, at(rel, wide, wide)],
            msend.at[s], arecv.at[s - first_groups], other_id,
        )

    def b_copy(s, group, row, rel):
        return remote(
            field.at[group, at(row, wide, wide)], rbuf.at[group, at(rel, wide, wide)],
            msend.at[s], brecv.at[s - first_groups], other_id,
        )

    def forward_copy(slot, group):
        return remote(field.at[group, at(row0, wide, wide)], ebuf.at[group], fsend.at[slot], frecv.at[slot], end_id)

    def norm_copy(i, peer):
        return remote(nbuf.at[2 * i], nbuf.at[2 * i + 1], nsend.at[i], nrecv.at[i], peer)

    def straight_copy(i, part, row_peer, peer):
        return pltpu.make_async_remote_copy(
            src_ref=straight.at[i, part, row_peer], dst_ref=late.at[i, t],
            send_sem=lsend.at[i], recv_sem=lrecv.at[i],
            device_id={"ta": row_peer, "sa": peer}, device_id_type=MESH,
        )

    def rows_copy(group, peer):
        return pltpu.make_async_remote_copy(
            src_ref=fin.at[group, peer], dst_ref=recv.at[group, t],
            send_sem=xsend.at[group], recv_sem=xrecv.at[group],
            device_id={"ta": peer}, device_id_type=MESH,
        )

    def angles(slot, plane):
        site = lax.broadcasted_iota(jnp.int32, (1, planes), 1)
        for p in range(moms):
            phase_index = (
                momenta_ref[0, p] * lax.rem(site, LX)
                + momenta_ref[1, p] * lax.div(site, LX)
                + momenta_ref[2, p] * plane
            )
            angle = jnp.mod(phase_index, LX).astype(jnp.float32) * (full_turn / LX)
            trig[slot, 0, p:p + 1] = jnp.cos(angle)
            trig[slot, 1, p:p + 1] = jnp.sin(angle)

    def phased(load, slot, store):
        for c in range(NC):
            re, im = load(c), load(NC + c)
            for p in range(moms):
                cosine, sine = trig[slot, 0, p:p + 1], trig[slot, 1, p:p + 1]
                store(p, c, (re * cosine + im * sine).astype(jnp.bfloat16))
                store(p, NC + c, (im * cosine - re * sine).astype(jnp.bfloat16))

    def own_part(group, k):
        return lown[at(group * tile, GV, GV), k * planes:(k + 1) * planes].astype(jnp.float32)

    def own_right(group, base):
        def store(p, k, value):
            rown[base + p * GV:base + (p + 1) * GV, k * planes:(k + 1) * planes] = value
        phased(lambda k: own_part(group, k), 0, store)

    def times(a, b):
        return lax.dot_general(a, b, (((1,), (1,)), ((), ())), preferred_element_type=jnp.float32)

    def split(value, ref):
        for peer in range(nta):
            for c in range(2):
                base = peer // per * tile + c * GV + peer % per * rows
                ref[peer, c] = value[base:base + rows]

    def finish(group, value):
        split(value * scale, fin.at[group])
        for j in range(1, nta):
            rows_copy(group, lax.rem(t + j, nta)).start()
        recv[group, t] = fin[group, t]

    lane = lax.broadcasted_iota(jnp.int32, (nta * rows, 128), 1) // GV

    def assemble(b, last):
        parts = []
        for g in range(ng):
            arrived = recv.at[b * ng + g, pl.ds(0, nta - 1)]
            pltpu.make_async_copy(arrived, arrived, xrecv.at[b * ng + g]).wait()
            if last:
                pltpu.make_async_copy(late.at[g], late.at[g], lrecv.at[g]).wait()
        for c in range(2):
            for g in range(ng):
                part = recv[b * ng + g, :, c].reshape(nta * rows, 128)
                if last:
                    part = part + late[g, :, c].reshape(nta * rows, 128)
                parts.append(part)
        d = moms // 2
        while d:
            keep = (lane // d) % 2 == 0
            later = list(parts)
            for i in range(moms):
                if (i // d) % 2 == 0:
                    low, high = parts[i], parts[i + d]
                    later[i] = jnp.where(keep, low, pltpu.roll(high, d * GV, 1))
                    later[i + d] = jnp.where(keep, pltpu.roll(low, 128 - d * GV, 1), high)
            parts = later
            d //= 2
        for p in range(moms):
            for source in range(nta):
                out_ref[p, b, :, source, :] = parts[p][source * rows:(source + 1) * rows]

    def drain_rows(group, carry):
        sent = recv.at[group, pl.ds(0, nta - 1)]
        pltpu.make_async_copy(sent, sent, xsend.at[group]).wait()
        return carry

    def norms():
        squares = []
        for b in range(NBLK):
            total = jnp.zeros((BS, 128), jnp.float32)
            for k in range(2 * NC):
                for at_lane in range(0, planes, 128):
                    value = ev_ref[k, b, :, at_lane:at_lane + 128].astype(jnp.float32)
                    total = total + value * value
            squares.append(total)
        nbuf[0] = lax.dot_general(
            jnp.ones((8, 128), jnp.float32), jnp.concatenate(squares, axis=0), (((1,), (1,)), ((), ())),
            precision=lax.Precision.HIGHEST, preferred_element_type=jnp.float32,
        )

    def build():
        for b in range(NBLK):
            stored = order_ref[b]
            for k in range(2 * NC):
                value = ev_ref[k, stored]
                mirror = (k + NC) % (2 * NC)
                turned = value if k < NC else -value
                for g in range(ng):
                    base = (b * ng + g) * tile
                    lown[base:base + GV, k * planes:(k + 1) * planes] = value[g * GV:(g + 1) * GV]
                    lown[base + GV:base + tile, mirror * planes:(mirror + 1) * planes] = turned[g * GV:(g + 1) * GV]

    @pl.when(is_end)
    def _():
        def widen(s, group):
            stored = order_ref[group // ng]
            for k in range(2 * NC):
                value = ev_ref[k, stored, at(lax.rem(group, ng) * GV, GV, GV), :]
                vsend[s, :, k * planes:(k + 1) * planes] = value.astype(jnp.float32)

        def widen_first(s, carry):
            widen(s, first(s, hi))
            return carry

        def widen_second(s, carry):
            widen(s, second(s, hi))
            return carry

        lax.fori_loop(0, ng, widen_first, 0)
        pl.semaphore_wait(barrier, 1)
        for s in range(ng):
            vector_copy(s).start()
        lax.fori_loop(ng, first_groups, widen_first, 0)
        norms()
        norm_copy(0, mid_id).start()
        for s in range(ng, first_groups):
            vector_copy(s).start()
        lax.fori_loop(first_groups, groups, widen_second, 0)
        for s in range(first_groups, groups):
            vector_copy(s).start()
        angles(0, z)
        build()

        def own(i, carry):
            for q in range(2):
                own_right(2 * i + q, q * 128)
            value = times(lown[at(row0, wide, wide), :], rown[...])
            for q in range(2):
                field[2 * i + q, at(row0, wide, wide)] = value[:, q * 128:(q + 1) * 128]
            return carry

        lax.fori_loop(0, first_groups, own, 0)

        def take(s, group):
            forward_copy(s, group).wait_recv()
            finish(group, field[group, at(row0, wide, wide)] + ebuf[group])

        def take_first(s, carry):
            take(s, first(s, 1 - hi))
            return carry

        def take_second(s, carry):
            take(s, second(s, 1 - hi))
            return carry

        lax.fori_loop(0, first_groups, take_first, 0)
        lax.fori_loop(groups - ng, groups, take_second, 0)

        def put(m, carry):
            assemble(blk(m, hi), False)
            return carry

        lax.fori_loop(0, 2, put, 0)
        lax.fori_loop(first_groups, groups - ng, take_second, 0)
        lax.fori_loop(2, NBLK - 1, put, 0)
        norm_copy(2, end_id).wait_recv()
        norm_ref[...] = nbuf[5, 0:1] * inv_count
        norm_copy(0, mid_id).wait_send()

        def drain(s, carry):
            vector_copy(s).wait_send()
            return carry

        lax.fori_loop(0, groups, drain, 0)
        lax.fori_loop(0, groups, drain_rows, 0)
        assemble(blk(NBLK - 1, hi), True)

    @pl.when(jnp.logical_not(is_end))
    def _():
        build()
        angles(0, z)
        angles(1, end_id)

        def own(i):
            pair = (first(i, hi), second(i + first_groups, hi))
            for q in range(2):
                own_right(pair[q], q * 128)
            value = times(lown[...], rown[...])
            for q in range(2):
                field[pair[q]] = value[:, q * 128:(q + 1) * 128]

        def arrive(s, group, rows_too=True):
            vector_copy(s).wait_recv()
            base = group * tile
            for k in range(2 * NC if rows_too else 0):
                value = vrecv[s, :, k * planes:(k + 1) * planes]
                mirror = (k + NC) % (2 * NC)
                turned = value if k < NC else -value
                lend[at(base, GV, GV), k * planes:(k + 1) * planes] = value.astype(jnp.bfloat16)
                lend[at(base + GV, GV, GV), mirror * planes:(mirror + 1) * planes] = turned.astype(jnp.bfloat16)

            def store(p, k, value):
                rend[s, p * GV:(p + 1) * GV, k * planes:(k + 1) * planes] = value
            phased(lambda k: vrecv[s, :, k * planes:(k + 1) * planes], 1, store)

        def first_step(s, carry):
            own(s)

            @pl.when(s == 0)
            def _():
                pl.semaphore_wait(barrier, nta + 1)
                for j in range(1, nta):
                    pl.semaphore_signal(ready, inc=1, device_id={"ta": lax.rem(t + j, nta)}, device_id_type=MESH)
                norms()
                pl.semaphore_wait(ready, nta - 1)

            group = first(s, hi)

            @pl.when(lax.rem(s, 2) == 0)
            def _():
                forward_copy(groups - ng + s // 2, group).start()

            arrive(s, group)
            value = times(lend[at(far, 2 * wide, 2 * wide), :], rend[s])
            for u in range(2 * ng):
                came = 2 * (u % ng) + (1 - u // ng) + hi * (2 * (u // ng) - 1)

                @pl.when(came <= s)
                def _():
                    field[group, at(far + u * tile, tile, tile)] += value[u * tile:(u + 1) * tile]
                    tile_copy(s, group, u * tile).start()

            row = group * tile
            rel = row - far

            def earlier(i, carry):
                before = first(i, hi)
                field[before, at(row, tile, tile)] += times(lend[at(row, tile, tile), :], rend[i])
                tile_copy(i, before, rel).start()
                return carry

            lax.fori_loop(0, s, earlier, 0)
            return carry

        lax.fori_loop(0, first_groups, first_step, 0)

        def far_rows(s, rows_too):
            group = second(s, hi)
            arrive(s, group, rows_too)
            field[group, at(far, 2 * wide, 2 * wide)] += times(lend[at(far, 2 * wide, 2 * wide), :], rend[s])
            return group

        def send_b(s):
            b_copy(s, second(s, hi), row2, rel2).start()

        def send_straight(i, part, group, row, peer):
            split(field[group, at(row, wide, wide)] * scale, straight.at[i, part])
            for j in range(nta):
                straight_copy(i, part, lax.rem(t + j, nta), peer).start()

        def straight_a(s):
            send_straight(s - (groups - ng), 0, second(s, hi), row3, n - 1 - end_id)

        def straight_b(s):
            send_straight(s - (groups - ng), 1, second(s, hi), row2, other_id)

        def pass_on(slot, group):
            field[group, at(row0, wide, wide)] += rbuf[group, at(got0, wide, wide)]
            forward_copy(slot, group).start()

        def take_a(s):
            group = second(s, 1 - hi)
            a_copy(s, group, row0, got0).wait_recv()
            pass_on(s, group)

        def take_b(s):
            group = second(s, 1 - hi)
            b_copy(s, group, row1, got1).wait_recv()
            field[group, at(row1, wide, wide)] += rbuf[group, at(got1, wide, wide)]
            finish(group, field[group, at(row1, wide, wide)])

        def take_first(s, carry):
            group = first(s, 1 - hi)
            arrived = rbuf.at[group]
            pltpu.make_async_copy(arrived, arrived, mrecv.at[s]).wait()
            pass_on(s, group)
            field[group, at(row1, wide, wide)] += rbuf[group, at(got1, wide, wide)]
            return carry

        def last_a(s, carry):
            take_a(s)
            return carry

        def second_step(s, carry):
            @pl.when(s == first_groups + 2)
            def _():
                lax.fori_loop(0, first_groups, take_first, 0)

            @pl.when(s == first_groups + 3)
            def _():
                lax.fori_loop(first_groups, first_groups + 2, last_a, 0)

            @pl.when(s == first_groups)
            def _():
                norm_copy(0, mid_id).wait_recv()
                nbuf[2] = nbuf[0] + nbuf[1]
                norm_copy(1, other_id).start()

            group = far_rows(s, True)
            a_copy(s, group, row3, rel3).start()

            send_b(s)
            return carry

        def last_b(s, carry):
            take_b(s)
            return carry

        def catch_up_all(later, odd_first, done):
            def catch_up(q, carry):
                odd = 2 * q + odd_first
                slot = later * (first_groups + q) + (1 - later) * odd
                before = later * second(first_groups + q, hi) + (1 - later) * first(odd, hi)
                field[before, at(row1, wide, wide)] += times(lend[at(row1, wide, wide), :], rend[slot])
                if done:
                    finish(before, field[before, at(row1, wide, wide)])
                return carry

            lax.fori_loop(0, ng, catch_up, 0)

        def third_step(s, carry):
            step = s - (groups - ng)

            @pl.when(step == 0)
            def _():
                norm_copy(1, other_id).wait_recv()
                total = nbuf[2] + nbuf[3]
                nbuf[4] = total
                norm_ref[...] = total[0:1] * inv_count
                norm_copy(2, end_id).start()

            @pl.when(step < 2)
            def _():
                take_a(s - 2)

            @pl.when(step < 2)
            def _():
                lax.fori_loop(2 * s - 2 * first_groups, 2 * s - 2 * first_groups + 2, last_b, 0)

            group = far_rows(s, False)
            straight_a(s)

            straight_b(s)
            near = lend[at(row1, wide, wide), :]
            finish(group, field[group, at(row1, wide, wide)] + times(near, rend[s]))

            @pl.when(step < 2)
            def _():
                catch_up_all(1 - step, 1 - step, True)
            return carry

        lax.fori_loop(first_groups, groups - ng, second_step, 0)
        catch_up_all(0, 1, False)
        lax.fori_loop(groups - ng, groups, third_step, 0)

        def put(m, carry):
            assemble(blk(m, hi), False)
            return carry

        lax.fori_loop(0, NBLK - 1, put, 0)
        norm_copy(1, other_id).wait_send()
        norm_copy(2, end_id).wait_send()

        def drain(s, carry):
            forward_copy(s, s).wait_send()
            return carry

        def drain_sums(s, carry):
            sent = rbuf.at[s]
            pltpu.make_async_copy(sent, sent, msend.at[s]).wait()
            return carry

        def drain_straight(i, carry):
            sent = straight.at[i]
            pltpu.make_async_copy(sent, sent, lsend.at[i]).wait()
            return carry

        lax.fori_loop(0, groups, drain, 0)
        lax.fori_loop(0, groups - ng, drain_sums, 0)
        lax.fori_loop(0, groups, drain_rows, 0)
        lax.fori_loop(0, ng, drain_straight, 0)
        assemble(blk(NBLK - 1, hi), True)


def pair_scratch(n, nta, moms, nv, planes):
    f32, bf16 = jnp.float32, jnp.bfloat16
    deep = 2 * NC * planes
    ng = BS // GV
    groups = NBLK * ng
    rows = BS // nta
    dma = pltpu.SemaphoreType.DMA
    return [
        pltpu.VMEM((2 * nv, deep), bf16),
        pltpu.VMEM((2 * nv, deep), bf16),
        pltpu.VMEM((256, deep), bf16),
        pltpu.VMEM((groups, moms * GV, deep), bf16),
        pltpu.VMEM((2, 2, moms, planes), f32),
        pltpu.VMEM((groups, GV, deep), f32),
        pltpu.VMEM((groups, GV, deep), f32),
        pltpu.VMEM((groups, 2 * nv, 128), f32),
        pltpu.VMEM((groups, nv, 128), f32),
        pltpu.VMEM((groups, 2 * BS, 128), f32),
        pltpu.VMEM((groups, nta, 2, rows, 128), f32),
        pltpu.VMEM((groups, nta, 2, rows, 128), f32),
        pltpu.VMEM((ng, 2, nta, 2, rows, 128), f32),
        pltpu.VMEM((ng, nta, 2, rows, 128), f32),
        pltpu.VMEM((6, 8, nv), f32),
        dma((groups,)), dma((groups,)), dma((groups,)), dma((groups // 2,)),
        dma((groups // 2,)), dma((groups // 2,)), dma((groups,)), dma((groups,)),
        dma((groups,)), dma((groups,)), dma((ng,)), dma((ng,)), dma((3,)), dma((3,)),
        pltpu.SemaphoreType.REGULAR,
    ]


def line_scratch(n, nta, moms, nv, planes):
    f32 = jnp.float32
    ppd = NBLK * NBLK // n
    rows = BS // nta
    dma = pltpu.SemaphoreType.DMA
    return [
        pltpu.VMEM((nv, 2 * NC * planes), jnp.bfloat16),
        pltpu.VMEM((2 * nv, 2 * NC * planes), jnp.bfloat16),
        pltpu.VMEM((moms, NBLK * NBLK, BS, 2 * BS), f32),
        pltpu.VMEM((moms, NBLK * NBLK, BS, 2 * BS), f32),
        pltpu.VMEM((moms, NBLK * NBLK, BS, 2 * BS), f32),
        pltpu.VMEM((moms, nta, ppd, rows, 2 * BS), f32),
        pltpu.VMEM((moms, nta, ppd, rows, 2 * BS), f32),
        pltpu.VMEM((n, 8, nv), f32),
        dma((moms, n)), dma((moms, n)), dma((moms, n)), dma((moms, n)),
        dma((moms,)), dma((moms,)), dma((n,)), dma((n,)),
    ]


def body(eigenvectors, momenta, block_order):
    planes = eigenvectors.shape[-1]
    n, nta = lax.axis_size("sa"), lax.axis_size("ta")
    moms = momenta.shape[0]
    nv = eigenvectors.shape[1]
    ppd = NBLK * NBLK // n
    rows = BS // nta
    stored = eigenvectors.reshape(NBLK, BS, 2 * NC, planes).transpose(2, 0, 1, 3)
    count = 2 * NC * n * planes
    f32 = jnp.float32
    vmem = pl.BlockSpec(memory_space=pltpu.VMEM)
    smem = pl.BlockSpec(memory_space=pltpu.SMEM)
    paired = n == NBLK == 4 and moms * GV == 128 and rows % 8 == 0 and GV % rows == 0
    kernel, scratch = (pair_kernel, pair_scratch) if paired else (line_kernel, line_scratch)
    fields, norms = pl.pallas_call(
        functools.partial(kernel, n, nta, 1.0 / math.sqrt(count), 1.0 / count),
        out_shape=(
            jax.ShapeDtypeStruct((moms, ppd, rows, nta, 2 * BS), f32),
            jax.ShapeDtypeStruct((1, nv), f32),
        ),
        in_specs=[smem, smem, vmem],
        out_specs=(vmem, vmem),
        scratch_shapes=scratch(n, nta, moms, nv, planes),
        compiler_params=pltpu.CompilerParams(collective_id=0, has_side_effects=True, vmem_limit_bytes=48 * 1024 * 1024),
    )(block_order, momenta.T, stored)
    return fields, norms


def solution(mesh):
    return jax.shard_map(
        body,
        mesh=mesh,
        in_specs=(P("ta", None, None, None, "sa", None), P(), P()),
        out_specs=(P(None, "sa", "ta", None, None), P("ta", None)),
        check_vma=False,
    )
```

```python
import functools
import math

import jax
import jax.numpy as jnp
from jax import lax
from jax.experimental import pallas as pl
from jax.experimental.pallas import tpu as pltpu
from jax.sharding import PartitionSpec as P

NC = 3
BS = 64
NBLK = 4
LX = 96
MESH = pl.DeviceIdType.MESH

full_turn = 2.0 * math.pi


def line_kernel(
    n, nta, scale, inv_count,
    order_ref, momenta_ref, ev_ref,
    out_ref, norm_ref,
    left, right, parts, rbuf, lbuf, final, recv, nbuf,
    rsend, rrecv, lsend, lrecv, asend, arecv, nsend, nrecv,
):
    t, z = lax.axis_index("ta"), lax.axis_index("sa")
    moms, planes = momenta_ref.shape[1], ev_ref.shape[-1]
    ppd = NBLK * NBLK // n
    rows = BS // nta
    half = NC * planes

    barrier = pltpu.get_barrier_semaphore()
    for j in range(1, n):
        pl.semaphore_signal(barrier, inc=1, device_id={"sa": lax.rem(z + j, n)}, device_id_type=MESH)
    for j in range(1, nta):
        pl.semaphore_signal(barrier, inc=1, device_id={"ta": lax.rem(t + j, nta)}, device_id_type=MESH)

    for b in range(NBLK):
        stored = order_ref[b]
        for k in range(2 * NC):
            left[b * BS:(b + 1) * BS, k * planes:(k + 1) * planes] = ev_ref[k, stored]
    def norm_copy(peer, slot):
        return pltpu.make_async_remote_copy(
            src_ref=nbuf.at[slot], dst_ref=nbuf.at[slot], send_sem=nsend.at[peer], recv_sem=nrecv.at[slot],
            device_id={"sa": peer}, device_id_type=MESH,
        )

    def shard(ref, p, s):
        return ref.at[p, pl.ds(s * ppd, ppd)]

    def rightward(src, p, s):
        return pltpu.make_async_remote_copy(
            src_ref=shard(src, p, s), dst_ref=shard(rbuf, p, s), send_sem=rsend.at[p, s], recv_sem=rrecv.at[p, s],
            device_id={"sa": lax.rem(z + 1, n)}, device_id_type=MESH,
        )

    def leftward(src, p, s):
        return pltpu.make_async_remote_copy(
            src_ref=shard(src, p, s), dst_ref=shard(lbuf, p, s), send_sem=lsend.at[p, s], recv_sem=lrecv.at[p, s],
            device_id={"sa": lax.rem(z + n - 1, n)}, device_id_type=MESH,
        )

    def compute(p):
        site = lax.broadcasted_iota(jnp.int32, (1, planes), 1)
        phase_index = (
            momenta_ref[0, p] * lax.rem(site, LX)
            + momenta_ref[1, p] * lax.div(site, LX)
            + momenta_ref[2, p] * z
        )
        angles = jnp.mod(phase_index, LX).astype(jnp.float32) * (full_turn / LX)
        cosine, sine = jnp.cos(angles), jnp.sin(angles)
        for c in range(NC):
            lanes = slice(c * planes, (c + 1) * planes)
            upper = slice(half + c * planes, half + (c + 1) * planes)
            for b in range(NBLK):
                re = left[b * BS:(b + 1) * BS, lanes].astype(jnp.float32)
                im = left[b * BS:(b + 1) * BS, upper].astype(jnp.float32)
                phased_re = (re * cosine + im * sine).astype(jnp.bfloat16)
                phased_im = (im * cosine - re * sine).astype(jnp.bfloat16)
                first = slice(2 * b * BS, (2 * b + 1) * BS)
                second = slice((2 * b + 1) * BS, (2 * b + 2) * BS)
                right[first, lanes] = phased_re
                right[first, upper] = phased_im
                right[second, lanes] = phased_im
                right[second, upper] = -phased_re
        for pair in range(NBLK // 2):
            product = lax.dot_general(
                left[...], right[pair * 4 * BS:(pair + 1) * 4 * BS, :], (((1,), (1,)), ((), ())),
                preferred_element_type=jnp.float32,
            )
            for a in range(NBLK):
                for b in range(2):
                    parts[p, a * NBLK + 2 * pair + b] = product[a * BS:(a + 1) * BS, b * 2 * BS:(b + 1) * 2 * BS]

    def open_lines(slot):
        @pl.when(z == 0)
        def _():
            for s in range(n - 1, 0, -1):
                p = slot - (n - 1 - s)

                @pl.when((p >= 0) & (p < moms))
                def _():
                    rightward(parts, p, s).start()

        @pl.when(z == n - 1)
        def _():
            for s in range(n - 1):
                p = slot - s

                @pl.when((p >= 0) & (p < moms))
                def _():
                    leftward(parts, p, s).start()

    def compute_and_open(p, carry):
        compute(p)
        open_lines(p)
        return carry

    def only_open(slot, carry):
        open_lines(slot)
        return carry

    compute(0)
    pl.semaphore_wait(barrier, n - 1 + nta - 1)
    open_lines(0)
    lax.fori_loop(1, moms, compute_and_open, 0)
    lax.fori_loop(moms, moms + n - 2, only_open, 0)

    squares = []
    for b in range(NBLK):
        total = jnp.zeros((BS, 128), jnp.float32)
        for k in range(2 * NC):
            for lane in range(0, planes, 128):
                value = ev_ref[k, b, :, lane:lane + 128].astype(jnp.float32)
                total = total + value * value
        squares.append(total)
    nbuf[z] = lax.dot_general(
        jnp.ones((8, 128), jnp.float32), jnp.concatenate(squares, axis=0), (((1,), (1,)), ((), ())),
        precision=lax.Precision.HIGHEST, preferred_element_type=jnp.float32,
    )

    for j in range(1, n):
        norm_copy(lax.rem(z + j, n), z).start()

    def rows_copy(p, peer):
        return pltpu.make_async_remote_copy(
            src_ref=final.at[p, peer], dst_ref=recv.at[p, t], send_sem=asend.at[p], recv_sem=arecv.at[p],
            device_id={"ta": peer}, device_id_type=MESH,
        )

    def step(i, carry):
        p_final = i - (n - 2)
        p_out = p_final - 1

        for s in range(n - 1, 0, -1):
            p_right = i - (z - 1) - (n - 1 - s)

            @pl.when((z > 0) & (s > z) & (p_right >= 0) & (p_right < moms))
            def _():
                copy = rightward(rbuf, p_right, s)
                copy.wait_recv()
                for k in range(ppd):
                    rbuf[p_right, s * ppd + k] += parts[p_right, s * ppd + k]
                copy.start()

        for s in range(n - 1):
            p_left = i - (n - 2 - z) - s

            @pl.when((z < n - 1) & (s < z) & (p_left >= 0) & (p_left < moms))
            def _():
                copy = leftward(lbuf, p_left, s)
                copy.wait_recv()
                for k in range(ppd):
                    lbuf[p_left, s * ppd + k] += parts[p_left, s * ppd + k]
                copy.start()

        @pl.when((p_final >= 0) & (p_final < moms))
        def _():
            @pl.when(z > 0)
            def _():
                rightward(rbuf, p_final, z).wait_recv()
                for k in range(ppd):
                    parts[p_final, z * ppd + k] += rbuf[p_final, z * ppd + k]

            @pl.when(z < n - 1)
            def _():
                leftward(lbuf, p_final, z).wait_recv()
                for k in range(ppd):
                    parts[p_final, z * ppd + k] += lbuf[p_final, z * ppd + k]

            for k in range(ppd):
                value = parts[p_final, z * ppd + k] * scale
                for peer in range(nta):
                    final[p_final, peer, k] = value[peer * rows:(peer + 1) * rows]
            for j in range(1, nta):
                rows_copy(p_final, lax.rem(t + j, nta)).start()
            recv[p_final, t] = final[p_final, t]

        @pl.when((p_out >= 0) & (p_out < moms))
        def _():
            arrived = recv.at[p_out, pl.ds(0, nta - 1)]
            pltpu.make_async_copy(arrived, arrived, arecv.at[p_out]).wait()
            for source in range(nta):
                for k in range(ppd):
                    out_ref[p_out, k, :, source, :] = recv[p_out, source, k]

        return carry

    lax.fori_loop(0, moms + n - 1, step, 0)

    for j in range(1, n):
        norm_copy(lax.rem(z + j, n), lax.rem(z + j, n)).wait_recv()
    total = nbuf[0]
    for q in range(1, n):
        total = total + nbuf[q]
    norm_ref[...] = total[0:1] * inv_count
    for j in range(1, n):
        norm_copy(lax.rem(z + j, n), z).wait_send()

    def drain(p, carry):
        for s in range(n):
            @pl.when(s > z)
            def _():
                rightward(parts, p, s).wait_send()

            @pl.when(s < z)
            def _():
                leftward(parts, p, s).wait_send()
        sent = final.at[p, pl.ds(0, nta - 1)]
        pltpu.make_async_copy(sent, sent, asend.at[p]).wait()
        return carry

    lax.fori_loop(0, moms, drain, 0)


GV = 16


def pair_kernel(
    n, nta, scale, inv_count,
    order_ref, momenta_ref, ev_ref,
    out_ref, norm_ref,
    lown, lend, rown, rend, trig, vsend, vrecv, field, rbuf, ebuf, fin, recv, straight, late, nbuf,
    vss, vrs, msend, mrecv, arecv, brecv, fsend, frecv, xsend, xrecv, lsend, lrecv, nsend, nrecv, ready,
):
    t, z = lax.axis_index("ta"), lax.axis_index("sa")
    moms, planes = momenta_ref.shape[1], ev_ref.shape[-1]
    half = NC * planes
    ng = BS // GV
    groups = NBLK * ng
    first_groups = groups // 2
    tile = 2 * GV
    wide = 2 * BS
    rows = BS // nta
    per = GV // rows
    hi = z // (n // 2)
    end_id = hi * (n - 1)
    mid_id = 1 + hi * (n - 3)
    other_id = n - 1 - z

    def blk(m, h):
        return m + h * (NBLK - 1 - 2 * m)

    def first(s, h):
        return blk(NBLK - 1 - lax.rem(s, 2), h) * ng + s // 2

    def second(s, h):
        return blk(NBLK - 1 - s // ng, h) * ng + lax.rem(s, ng)

    def at(start, size, step):
        return pl.ds(pl.multiple_of(start, step), size)

    row0, row1 = blk(0, hi) * wide, blk(1, hi) * wide
    row3 = blk(NBLK - 1, hi) * wide
    row2 = blk(NBLK - 2, hi) * wide
    far = (1 - hi) * 2 * wide
    rel3, rel2 = (1 - hi) * wide, hi * wide
    got0, got1 = hi * wide, (1 - hi) * wide

    barrier = pltpu.get_barrier_semaphore()
    is_end = lax.rem(z, n - 1) == 0

    @pl.when(is_end)
    def _():
        pl.semaphore_signal(barrier, inc=1, device_id={"sa": mid_id}, device_id_type=MESH)

    @pl.when(jnp.logical_not(is_end))
    def _():
        for peer in (end_id, other_id):
            pl.semaphore_signal(barrier, inc=1, device_id={"sa": peer}, device_id_type=MESH)
        for j in range(1, nta):
            pl.semaphore_signal(barrier, inc=1, device_id={"ta": lax.rem(t + j, nta)}, device_id_type=MESH)

    def remote(src, dst, send_sem, recv_sem, peer):
        return pltpu.make_async_remote_copy(
            src_ref=src, dst_ref=dst, send_sem=send_sem, recv_sem=recv_sem,
            device_id={"sa": peer}, device_id_type=MESH,
        )

    def vector_copy(s):
        return remote(vsend.at[s], vrecv.at[s], vss.at[s], vrs.at[s], mid_id)

    def tile_copy(slot, group, rel):
        return remote(
            field.at[group, at(far + rel, tile, tile)], rbuf.at[group, at(rel, tile, tile)],
            msend.at[slot], mrecv.at[lax.rem(slot, first_groups)], other_id,
        )

    def a_copy(s, group, row, rel):
        return remote(
            field.at[group, at(row, wide, wide)], rbuf.at[group, at(rel, wide, wide)],
            msend.at[s], arecv.at[s - first_groups], other_id,
        )

    def b_copy(s, group, row, rel):
        return remote(
            field.at[group, at(row, wide, wide)], rbuf.at[group, at(rel, wide, wide)],
            msend.at[s], brecv.at[s - first_groups], other_id,
        )

    def forward_copy(slot, group):
        return remote(field.at[group, at(row0, wide, wide)], ebuf.at[group], fsend.at[slot], frecv.at[slot], end_id)

    def norm_copy(i, peer):
        return remote(nbuf.at[2 * i], nbuf.at[2 * i + 1], nsend.at[i], nrecv.at[i], peer)

    def straight_copy(i, part, row_peer, peer):
        return pltpu.make_async_remote_copy(
            src_ref=straight.at[i, part, row_peer], dst_ref=late.at[i, t],
            send_sem=lsend.at[i], recv_sem=lrecv.at[i],
            device_id={"ta": row_peer, "sa": peer}, device_id_type=MESH,
        )

    def rows_copy(group, peer):
        return pltpu.make_async_remote_copy(
            src_ref=fin.at[group, peer], dst_ref=recv.at[group, t],
            send_sem=xsend.at[group], recv_sem=xrecv.at[group],
            device_id={"ta": peer}, device_id_type=MESH,
        )

    def angles(slot, plane):
        site = lax.broadcasted_iota(jnp.int32, (1, planes), 1)
        for p in range(moms):
            phase_index = (
                momenta_ref[0, p] * lax.rem(site, LX)
                + momenta_ref[1, p] * lax.div(site, LX)
                + momenta_ref[2, p] * plane
            )
            angle = jnp.mod(phase_index, LX).astype(jnp.float32) * (full_turn / LX)
            trig[slot, 0, p:p + 1] = jnp.cos(angle)
            trig[slot, 1, p:p + 1] = jnp.sin(angle)

    def phased(load, slot, store):
        for c in range(NC):
            re, im = load(c), load(NC + c)
            for p in range(moms):
                cosine, sine = trig[slot, 0, p:p + 1], trig[slot, 1, p:p + 1]
                store(p, c, (re * cosine + im * sine).astype(jnp.bfloat16))
                store(p, NC + c, (im * cosine - re * sine).astype(jnp.bfloat16))

    def own_part(group, k):
        return lown[at(group * tile, GV, GV), k * planes:(k + 1) * planes].astype(jnp.float32)

    def own_right(group, base):
        def store(p, k, value):
            rown[base + p * GV:base + (p + 1) * GV, k * planes:(k + 1) * planes] = value
        phased(lambda k: own_part(group, k), 0, store)

    def times(a, b):
        return lax.dot_general(a, b, (((1,), (1,)), ((), ())), preferred_element_type=jnp.float32)

    def split(value, ref):
        for peer in range(nta):
            for c in range(2):
                base = peer // per * tile + c * GV + peer % per * rows
                ref[peer, c] = value[base:base + rows]

    def finish(group, value):
        split(value * scale, fin.at[group])
        for j in range(1, nta):
            rows_copy(group, lax.rem(t + j, nta)).start()
        recv[group, t] = fin[group, t]

    lane = lax.broadcasted_iota(jnp.int32, (nta * rows, 128), 1) // GV

    def assemble(b, last):
        parts = []
        for g in range(ng):
            arrived = recv.at[b * ng + g, pl.ds(0, nta - 1)]
            pltpu.make_async_copy(arrived, arrived, xrecv.at[b * ng + g]).wait()
            if last:
                pltpu.make_async_copy(late.at[g], late.at[g], lrecv.at[g]).wait()
        for c in range(2):
            for g in range(ng):
                part = recv[b * ng + g, :, c].reshape(nta * rows, 128)
                if last:
                    part = part + late[g, :, c].reshape(nta * rows, 128)
                parts.append(part)
        d = moms // 2
        while d:
            keep = (lane // d) % 2 == 0
            later = list(parts)
            for i in range(moms):
                if (i // d) % 2 == 0:
                    low, high = parts[i], parts[i + d]
                    later[i] = jnp.where(keep, low, pltpu.roll(high, d * GV, 1))
                    later[i + d] = jnp.where(keep, pltpu.roll(low, 128 - d * GV, 1), high)
            parts = later
            d //= 2
        for p in range(moms):
            for source in range(nta):
                out_ref[p, b, :, source, :] = parts[p][source * rows:(source + 1) * rows]

    def drain_rows(group, carry):
        sent = recv.at[group, pl.ds(0, nta - 1)]
        pltpu.make_async_copy(sent, sent, xsend.at[group]).wait()
        return carry

    def norms():
        squares = []
        for b in range(NBLK):
            total = jnp.zeros((BS, 128), jnp.float32)
            for k in range(2 * NC):
                for at_lane in range(0, planes, 128):
                    value = ev_ref[k, b, :, at_lane:at_lane + 128].astype(jnp.float32)
                    total = total + value * value
            squares.append(total)
        nbuf[0] = lax.dot_general(
            jnp.ones((8, 128), jnp.float32), jnp.concatenate(squares, axis=0), (((1,), (1,)), ((), ())),
            precision=lax.Precision.HIGHEST, preferred_element_type=jnp.float32,
        )

    def build():
        for b in range(NBLK):
            stored = order_ref[b]
            for k in range(2 * NC):
                value = ev_ref[k, stored]
                mirror = (k + NC) % (2 * NC)
                turned = value if k < NC else -value
                for g in range(ng):
                    base = (b * ng + g) * tile
                    lown[base:base + GV, k * planes:(k + 1) * planes] = value[g * GV:(g + 1) * GV]
                    lown[base + GV:base + tile, mirror * planes:(mirror + 1) * planes] = turned[g * GV:(g + 1) * GV]

    @pl.when(is_end)
    def _():
        def widen(s, group):
            stored = order_ref[group // ng]
            for k in range(2 * NC):
                value = ev_ref[k, stored, at(lax.rem(group, ng) * GV, GV, GV), :]
                vsend[s, :, k * planes:(k + 1) * planes] = value.astype(jnp.float32)

        def widen_first(s, carry):
            widen(s, first(s, hi))
            return carry

        def widen_second(s, carry):
            widen(s, second(s, hi))
            return carry

        lax.fori_loop(0, ng, widen_first, 0)
        pl.semaphore_wait(barrier, 1)
        for s in range(ng):
            vector_copy(s).start()
        lax.fori_loop(ng, first_groups, widen_first, 0)
        norms()
        norm_copy(0, mid_id).start()
        for s in range(ng, first_groups):
            vector_copy(s).start()
        lax.fori_loop(first_groups, groups, widen_second, 0)
        for s in range(first_groups, groups):
            vector_copy(s).start()
        angles(0, z)
        build()

        def own(i, carry):
            for q in range(2):
                own_right(2 * i + q, q * 128)
            value = times(lown[at(row0, wide, wide), :], rown[...])
            for q in range(2):
                field[2 * i + q, at(row0, wide, wide)] = value[:, q * 128:(q + 1) * 128]
            return carry

        lax.fori_loop(0, first_groups, own, 0)

        def take(s, group):
            forward_copy(s, group).wait_recv()
            finish(group, field[group, at(row0, wide, wide)] + ebuf[group])

        def take_first(s, carry):
            take(s, first(s, 1 - hi))
            return carry

        def take_second(s, carry):
            take(s, second(s, 1 - hi))
            return carry

        lax.fori_loop(0, first_groups, take_first, 0)
        lax.fori_loop(groups - ng, groups, take_second, 0)

        def put(m, carry):
            assemble(blk(m, hi), False)
            return carry

        lax.fori_loop(0, 2, put, 0)
        lax.fori_loop(first_groups, groups - ng, take_second, 0)
        lax.fori_loop(2, NBLK - 1, put, 0)
        norm_copy(2, end_id).wait_recv()
        norm_ref[...] = nbuf[5, 0:1] * inv_count
        norm_copy(0, mid_id).wait_send()

        def drain(s, carry):
            vector_copy(s).wait_send()
            return carry

        lax.fori_loop(0, groups, drain, 0)
        lax.fori_loop(0, groups, drain_rows, 0)
        assemble(blk(NBLK - 1, hi), True)

    @pl.when(jnp.logical_not(is_end))
    def _():
        build()
        angles(0, z)
        angles(1, end_id)

        def own(i):
            pair = (first(i, hi), second(i + first_groups, hi))
            for q in range(2):
                own_right(pair[q], q * 128)
            value = times(lown[...], rown[...])
            for q in range(2):
                field[pair[q]] = value[:, q * 128:(q + 1) * 128]

        def arrive(s, group, rows_too=True):
            vector_copy(s).wait_recv()
            base = group * tile
            for k in range(2 * NC if rows_too else 0):
                value = vrecv[s, :, k * planes:(k + 1) * planes]
                mirror = (k + NC) % (2 * NC)
                turned = value if k < NC else -value
                lend[at(base, GV, GV), k * planes:(k + 1) * planes] = value.astype(jnp.bfloat16)
                lend[at(base + GV, GV, GV), mirror * planes:(mirror + 1) * planes] = turned.astype(jnp.bfloat16)

            def store(p, k, value):
                rend[s, p * GV:(p + 1) * GV, k * planes:(k + 1) * planes] = value
            phased(lambda k: vrecv[s, :, k * planes:(k + 1) * planes], 1, store)

        def first_step(s, carry):
            own(s)

            @pl.when(s == 0)
            def _():
                pl.semaphore_wait(barrier, nta + 1)
                for j in range(1, nta):
                    pl.semaphore_signal(ready, inc=1, device_id={"ta": lax.rem(t + j, nta)}, device_id_type=MESH)
                norms()
                pl.semaphore_wait(ready, nta - 1)

            group = first(s, hi)

            @pl.when(lax.rem(s, 2) == 0)
            def _():
                forward_copy(groups - ng + s // 2, group).start()

            arrive(s, group)
            value = times(lend[at(far, 2 * wide, 2 * wide), :], rend[s])
            for u in range(2 * ng):
                came = 2 * (u % ng) + (1 - u // ng) + hi * (2 * (u // ng) - 1)

                @pl.when(came <= s)
                def _():
                    field[group, at(far + u * tile, tile, tile)] += value[u * tile:(u + 1) * tile]
                    tile_copy(s, group, u * tile).start()

            row = group * tile
            rel = row - far

            def earlier(i, carry):
                before = first(i, hi)
                field[before, at(row, tile, tile)] += times(lend[at(row, tile, tile), :], rend[i])
                tile_copy(i, before, rel).start()
                return carry

            lax.fori_loop(0, s, earlier, 0)
            return carry

        lax.fori_loop(0, first_groups, first_step, 0)

        def far_rows(s, rows_too):
            group = second(s, hi)
            arrive(s, group, rows_too)
            field[group, at(far, 2 * wide, 2 * wide)] += times(lend[at(far, 2 * wide, 2 * wide), :], rend[s])
            return group

        def send_b(s):
            b_copy(s, second(s, hi), row2, rel2).start()

        def send_straight(i, part, group, row, peer):
            split(field[group, at(row, wide, wide)] * scale, straight.at[i, part])
            for j in range(nta):
                straight_copy(i, part, lax.rem(t + j, nta), peer).start()

        def straight_a(s):
            send_straight(s - (groups - ng), 0, second(s, hi), row3, n - 1 - end_id)

        def straight_b(s):
            send_straight(s - (groups - ng), 1, second(s, hi), row2, other_id)

        def pass_on(slot, group):
            field[group, at(row0, wide, wide)] += rbuf[group, at(got0, wide, wide)]
            forward_copy(slot, group).start()

        def take_a(s):
            group = second(s, 1 - hi)
            a_copy(s, group, row0, got0).wait_recv()
            pass_on(s, group)

        def take_b(s):
            group = second(s, 1 - hi)
            b_copy(s, group, row1, got1).wait_recv()
            field[group, at(row1, wide, wide)] += rbuf[group, at(got1, wide, wide)]
            finish(group, field[group, at(row1, wide, wide)])

        def take_first(s, carry):
            group = first(s, 1 - hi)
            arrived = rbuf.at[group]
            pltpu.make_async_copy(arrived, arrived, mrecv.at[s]).wait()
            pass_on(s, group)
            field[group, at(row1, wide, wide)] += rbuf[group, at(got1, wide, wide)]
            return carry

        def last_a(s, carry):
            take_a(s)
            return carry

        def second_step(s, carry):
            @pl.when(s == first_groups + 2)
            def _():
                lax.fori_loop(0, first_groups, take_first, 0)

            @pl.when(s == first_groups + 3)
            def _():
                lax.fori_loop(first_groups, first_groups + 2, last_a, 0)

            @pl.when(s == first_groups)
            def _():
                norm_copy(0, mid_id).wait_recv()
                nbuf[2] = nbuf[0] + nbuf[1]
                norm_copy(1, other_id).start()

            group = far_rows(s, True)
            a_copy(s, group, row3, rel3).start()

            send_b(s)
            return carry

        def last_b(s, carry):
            take_b(s)
            return carry

        def catch_up_all(later, odd_first, done):
            def catch_up(q, carry):
                odd = 2 * q + odd_first
                slot = later * (first_groups + q) + (1 - later) * odd
                before = later * second(first_groups + q, hi) + (1 - later) * first(odd, hi)
                field[before, at(row1, wide, wide)] += times(lend[at(row1, wide, wide), :], rend[slot])
                if done:
                    finish(before, field[before, at(row1, wide, wide)])
                return carry

            lax.fori_loop(0, ng, catch_up, 0)

        def third_step(s, carry):
            step = s - (groups - ng)

            @pl.when(step == 0)
            def _():
                norm_copy(1, other_id).wait_recv()
                total = nbuf[2] + nbuf[3]
                nbuf[4] = total
                norm_ref[...] = total[0:1] * inv_count
                norm_copy(2, end_id).start()

            @pl.when(step < 2)
            def _():
                take_a(s - 2)

            @pl.when(step < 2)
            def _():
                lax.fori_loop(2 * s - 2 * first_groups, 2 * s - 2 * first_groups + 2, last_b, 0)

            group = second(s, hi)
            arrive(s, group, False)
            for row, send in ((row3, straight_a), (row2, straight_b)):
                field[group, at(row, wide, wide)] += times(lend[at(row, wide, wide), :], rend[s])
                send(s)
            near = lend[at(row1, wide, wide), :]
            finish(group, field[group, at(row1, wide, wide)] + times(near, rend[s]))

            @pl.when(step < 2)
            def _():
                catch_up_all(1 - step, 1 - step, True)
            return carry

        lax.fori_loop(first_groups, groups - ng, second_step, 0)
        catch_up_all(0, 1, False)
        lax.fori_loop(groups - ng, groups, third_step, 0)

        def put(m, carry):
            assemble(blk(m, hi), False)
            return carry

        lax.fori_loop(0, NBLK - 1, put, 0)
        norm_copy(1, other_id).wait_send()
        norm_copy(2, end_id).wait_send()

        def drain(s, carry):
            forward_copy(s, s).wait_send()
            return carry

        def drain_sums(s, carry):
            sent = rbuf.at[s]
            pltpu.make_async_copy(sent, sent, msend.at[s]).wait()
            return carry

        def drain_straight(i, carry):
            sent = straight.at[i]
            pltpu.make_async_copy(sent, sent, lsend.at[i]).wait()
            return carry

        lax.fori_loop(0, groups, drain, 0)
        lax.fori_loop(0, groups - ng, drain_sums, 0)
        lax.fori_loop(0, groups, drain_rows, 0)
        lax.fori_loop(0, ng, drain_straight, 0)
        assemble(blk(NBLK - 1, hi), True)


def pair_scratch(n, nta, moms, nv, planes):
    f32, bf16 = jnp.float32, jnp.bfloat16
    deep = 2 * NC * planes
    ng = BS // GV
    groups = NBLK * ng
    rows = BS // nta
    dma = pltpu.SemaphoreType.DMA
    return [
        pltpu.VMEM((2 * nv, deep), bf16),
        pltpu.VMEM((2 * nv, deep), bf16),
        pltpu.VMEM((256, deep), bf16),
        pltpu.VMEM((groups, moms * GV, deep), bf16),
        pltpu.VMEM((2, 2, moms, planes), f32),
        pltpu.VMEM((groups, GV, deep), f32),
        pltpu.VMEM((groups, GV, deep), f32),
        pltpu.VMEM((groups, 2 * nv, 128), f32),
        pltpu.VMEM((groups, nv, 128), f32),
        pltpu.VMEM((groups, 2 * BS, 128), f32),
        pltpu.VMEM((groups, nta, 2, rows, 128), f32),
        pltpu.VMEM((groups, nta, 2, rows, 128), f32),
        pltpu.VMEM((ng, 2, nta, 2, rows, 128), f32),
        pltpu.VMEM((ng, nta, 2, rows, 128), f32),
        pltpu.VMEM((6, 8, nv), f32),
        dma((groups,)), dma((groups,)), dma((groups,)), dma((groups // 2,)),
        dma((groups // 2,)), dma((groups // 2,)), dma((groups,)), dma((groups,)),
        dma((groups,)), dma((groups,)), dma((ng,)), dma((ng,)), dma((3,)), dma((3,)),
        pltpu.SemaphoreType.REGULAR,
    ]


def line_scratch(n, nta, moms, nv, planes):
    f32 = jnp.float32
    ppd = NBLK * NBLK // n
    rows = BS // nta
    dma = pltpu.SemaphoreType.DMA
    return [
        pltpu.VMEM((nv, 2 * NC * planes), jnp.bfloat16),
        pltpu.VMEM((2 * nv, 2 * NC * planes), jnp.bfloat16),
        pltpu.VMEM((moms, NBLK * NBLK, BS, 2 * BS), f32),
        pltpu.VMEM((moms, NBLK * NBLK, BS, 2 * BS), f32),
        pltpu.VMEM((moms, NBLK * NBLK, BS, 2 * BS), f32),
        pltpu.VMEM((moms, nta, ppd, rows, 2 * BS), f32),
        pltpu.VMEM((moms, nta, ppd, rows, 2 * BS), f32),
        pltpu.VMEM((n, 8, nv), f32),
        dma((moms, n)), dma((moms, n)), dma((moms, n)), dma((moms, n)),
        dma((moms,)), dma((moms,)), dma((n,)), dma((n,)),
    ]


def body(eigenvectors, momenta, block_order):
    planes = eigenvectors.shape[-1]
    n, nta = lax.axis_size("sa"), lax.axis_size("ta")
    moms = momenta.shape[0]
    nv = eigenvectors.shape[1]
    ppd = NBLK * NBLK // n
    rows = BS // nta
    stored = eigenvectors.reshape(NBLK, BS, 2 * NC, planes).transpose(2, 0, 1, 3)
    count = 2 * NC * n * planes
    f32 = jnp.float32
    vmem = pl.BlockSpec(memory_space=pltpu.VMEM)
    smem = pl.BlockSpec(memory_space=pltpu.SMEM)
    paired = n == NBLK == 4 and moms * GV == 128 and rows % 8 == 0 and GV % rows == 0
    kernel, scratch = (pair_kernel, pair_scratch) if paired else (line_kernel, line_scratch)
    fields, norms = pl.pallas_call(
        functools.partial(kernel, n, nta, 1.0 / math.sqrt(count), 1.0 / count),
        out_shape=(
            jax.ShapeDtypeStruct((moms, ppd, rows, nta, 2 * BS), f32),
            jax.ShapeDtypeStruct((1, nv), f32),
        ),
        in_specs=[smem, smem, vmem],
        out_specs=(vmem, vmem),
        scratch_shapes=scratch(n, nta, moms, nv, planes),
        compiler_params=pltpu.CompilerParams(collective_id=0, has_side_effects=True, vmem_limit_bytes=48 * 1024 * 1024),
    )(block_order, momenta.T, stored)
    return fields, norms


def solution(mesh):
    return jax.shard_map(
        body,
        mesh=mesh,
        in_specs=(P("ta", None, None, None, "sa", None), P(), P()),
        out_specs=(P(None, "sa", "ta", None, None), P("ta", None)),
        check_vma=False,
    )
```
